32 devices in a mesh: grp: 2 (over y), gz: 4 (over z), gx: 2 (over x), row: 2 (over core).
Axes of the slice: x: 2, y: 2, z: 4, core: 2. Of those that a mesh axis runs over, the one named last changes fastest.
Arguments:
- volume: float32 [32, 512, 512], P(('grp', 'gz'), 'gx', 'row'), parts along dimension 0, may hold values from -6 to 6
- tile_table: bfloat16 [64, 128, 128], replicated, may hold values from -0.09375 to 0.09375
- tile_ids: int32 [4, 2, 2, 4, 32], P('gz', 'gx', 'row'), may hold values from 0 to 63
- block_ids: int32 [4, 2, 2, 4, 768], P('gz', 'gx', 'row'), may hold values from 0 to 2047
- live_slots: int32 [4, 2, 2, 4], P('gz', 'gx', 'row'), may hold values from 4 to 32, as said below
- measured: float32 [8, 512, 16], P(('grp', 'gz'), ('gx', 'row')), parts along dimension 0, may hold values from -12 to 12
- row_norm: float32 [4, 512, 16], P('gz', ('gx', 'row')), may hold values from 0.2 to 1
- col_norm: float32 [16, 512, 512], P('gz', 'gx', 'row'), may hold values from 0.5 to 2
Outputs:
- new_volume: float32 [32, 512, 512], P(('grp', 'gz'), 'gx', 'row'), parts along dimension 0
The draws below stay inside these ranges and needn't reach their ends.
There are 2 independent parts, one for each index of `grp`. The reference program is written for one: setup_inputs(seed, part) draws one part's arguments, and reference() takes and returns one part's arrays. A program takes and returns all parts, laid end to end along the dimension named above; an argument that names none is the same for every part. Nothing has to cross between parts.
Inputs may be any that keep to these rules, and one draw needn't show every extreme that they name: `block_ids`: indices of voxel blocks of the piece itself. `live_slots`: 32 is reached by some angle of some piece in every draw.
All inputs are finite; a program needn't handle non-finite values.
Results may differ from the reference program's by a relative error of at most 0.004.
Values may be sent and summed in bfloat16 or wider, within the bound.
No kernel may reach another device: no remote copies, remote signals or barrier semaphores. Data moves between devices by JAX's collectives and lax.ppermute only.
A program may use at most 64 MiB of HBM per device.

```python
import math
import jax
import jax.numpy as jnp
from jax import lax

SIDE = 512
DET_U = 512
TILE = 128
SLAB_Z = 4
SLOTS = 32
NTILES = 64
SLABS = 4
COLS = 2
HALVES = 2
ANGLES = 4
NZ = 16
WIN = 6
UBLK = 4
XCOL = 256
YHALF = 256
NBLK = 2048


def draw_live_slots(key, part):
    key_caps, key_top, key_fill, key_angle = jax.random.split(key, 4)
    piece_count = SLABS * COLS * HALVES
    least_cap = max(1, SLOTS // 4)
    piece_caps = jax.random.randint(key_caps, (piece_count,), least_cap, SLOTS + 1)
    top_piece = jax.random.randint(key_top, (), 0, piece_count)
    piece_caps = jnp.where(jnp.arange(piece_count) == top_piece, SLOTS, piece_caps)
    lower_bound = (piece_caps + 1) // 2
    random_bits = jax.random.randint(key_fill, (piece_count, ANGLES), 0, 1 << 20)
    counts = lower_bound[:, None] + random_bits % (piece_caps - lower_bound + 1)[:, None]
    top_angle = jax.random.randint(key_angle, (piece_count,), 0, ANGLES)
    counts = jnp.where(jnp.arange(ANGLES)[None, :] == top_angle[:, None], piece_caps[:, None], counts)
    return counts.reshape(SLABS, COLS, HALVES, ANGLES).astype(jnp.int32)


def place_ends(values, key, least, high):
    spot = [jax.random.randint(jax.random.fold_in(key, axis), (), 0, length) for axis, length in enumerate(values.shape)]
    widest = values.shape.index(max(values.shape))
    beside = spot[:widest] + [(spot[widest] + 1) % values.shape[widest]] + spot[widest + 1:]
    return values.at[tuple(spot)].set(least).at[tuple(beside)].set(high)


def shard_levels(own_key, extent, cuts, least, largest):
    def one(axis_at, parts):
        heights = jax.random.uniform(jax.random.fold_in(jax.random.fold_in(own_key, 6), axis_at), (parts,), jnp.float32, least / len(cuts), largest / len(cuts))
        return jnp.repeat(jnp.exp(heights), extent[axis_at] // parts).reshape((-1,) + (1,) * (len(extent) - axis_at - 1))

    loudness = one(*cuts[0])
    for cut in cuts[1:]:
        loudness = loudness * one(*cut)
    return loudness


def gaussian(stream_key, extent, scale, bound, cuts=(), kind=jnp.bfloat16):
    drawn = scale * jax.random.normal(stream_key, extent, jnp.float32)
    if cuts:
        drawn = drawn * shard_levels(stream_key, extent, cuts, -0.22, 0.18)
    return jnp.clip(drawn, -bound, bound).astype(kind)


def setup_inputs(seed: int = 0, part: int = 0) -> dict:
    key_list = jax.random.split(jax.random.key(seed), 9)
    part_keys = jax.random.split(jax.random.fold_in(key_list[8], part), 9)
    return {
        "volume": gaussian(part_keys[0], (NZ, SIDE, SIDE), 1.0, 6.0, ((0, 4), (1, 2), (2, 2)), jnp.float32),
        "tile_table": gaussian(key_list[1], (NTILES, TILE, TILE), (SLOTS * TILE) ** -0.5, 0.09375),
        "tile_ids": place_ends(jax.random.randint(key_list[2], (SLABS, COLS, HALVES, ANGLES, SLOTS), 0, NTILES), jax.random.fold_in(key_list[2], 1), 0, NTILES - 1).astype(jnp.int32),
        "block_ids": place_ends(jax.random.randint(key_list[3], (SLABS, COLS, HALVES, ANGLES, SLOTS * WIN * UBLK), 0, NBLK), jax.random.fold_in(key_list[3], 1), 0, NBLK - 1).astype(jnp.int32),
        "live_slots": draw_live_slots(jax.random.fold_in(key_list[8], 71), part),
        "measured": gaussian(part_keys[5], (ANGLES, DET_U, NZ), 2.0, 12.0, ((0, 4), (1, 4)), jnp.float32),
        "row_norm": jnp.clip(jnp.exp(math.log(1.0) - 1.609438 * jax.random.uniform(key_list[6], (ANGLES, DET_U, NZ), jnp.float32) ** shard_levels(key_list[6], (ANGLES, DET_U, NZ), ((0, 4), (1, 4)), -0.2, 0.2)), 0.2, 1.0),
        "col_norm": jnp.clip(jnp.exp(math.log(2.0) - 1.3862944 * jax.random.uniform(key_list[7], (NZ, SIDE, SIDE), jnp.float32) ** shard_levels(key_list[7], (NZ, SIDE, SIDE), ((0, 4), (1, 2), (2, 2)), -0.2, 0.2)), 0.5, 2.0),
    }


def reference(volume, tile_table, tile_ids, block_ids, live_slots, measured, row_norm, col_norm):
    piece_count = SLABS * COLS * HALVES
    pieces = volume.reshape(SLABS, SLAB_Z, COLS, XCOL, HALVES, YHALF).transpose(0, 2, 4, 1, 3, 5)
    voxel_rows = pieces.reshape(piece_count, NBLK, TILE).astype(jnp.bfloat16)
    tile_rows = tile_ids.reshape(piece_count, ANGLES, SLOTS)
    block_rows = block_ids.reshape(piece_count, ANGLES, SLOTS, WIN, UBLK)
    position = jnp.arange(SLOTS, dtype=jnp.int32)
    slot_mask = (position[None, None, :] < live_slots.reshape(piece_count, ANGLES)[:, :, None]).astype(jnp.float32)

    def forward(inputs):
        voxel_piece, tile_piece, block_piece, mask_piece = inputs
        picked = tile_table[tile_piece].astype(jnp.float32)
        voxels = voxel_piece[block_piece].astype(jnp.float32)
        return jnp.einsum("akdv,akwqv,ak->awqd", picked, voxels, mask_piece)

    partial_value = lax.map(forward, (voxel_rows, tile_rows, block_rows, slot_mask))
    per_slab = partial_value.reshape(SLABS, COLS * HALVES, ANGLES, WIN, DET_U).sum(axis=1)
    middle = per_slab[:, :, 1:SLAB_Z + 1]
    lower_rim = middle[:, :, 0].at[1:].add(per_slab[:-1, :, SLAB_Z + 1])
    upper_rim = middle[:, :, SLAB_Z - 1].at[:-1].add(per_slab[1:, :, 0])
    middle = middle.at[:, :, 0].set(lower_rim).at[:, :, SLAB_Z - 1].set(upper_rim)
    projection = middle.transpose(1, 3, 0, 2).reshape(ANGLES, DET_U, NZ)
    residual = (row_norm * (measured - projection)).astype(jnp.bfloat16)
    padded = jnp.pad(residual, ((0, 0), (0, 0), (1, 1)))
    head_rows = padded[:, :, :NZ].reshape(ANGLES, DET_U, SLABS, SLAB_Z)
    tail_rows = padded[:, :, 2:].reshape(ANGLES, DET_U, SLABS, SLAB_Z)[:, :, :, SLAB_Z - 2:]
    windows = jnp.concatenate([head_rows, tail_rows], axis=3).transpose(2, 0, 3, 1)
    windows = windows.reshape(SLABS, ANGLES, WIN, UBLK, TILE)
    piece_windows = jnp.repeat(windows, COLS * HALVES, axis=0)

    def backward(inputs):
        tile_piece, block_piece, mask_piece, window_piece = inputs
        picked = tile_table[tile_piece].astype(jnp.float32)
        spread = jnp.einsum("akdv,awqd,ak->akwqv", picked, window_piece.astype(jnp.float32), mask_piece)
        return jnp.zeros((NBLK, TILE), jnp.float32).at[block_piece].add(spread)

    back_sum = lax.map(backward, (tile_rows, block_rows, slot_mask, piece_windows))
    back_sum = back_sum.reshape(SLABS, COLS, HALVES, SLAB_Z, XCOL, YHALF).transpose(0, 3, 1, 4, 2, 5)
    return volume + col_norm * back_sum.reshape(NZ, SIDE, SIDE)
```

```python
import functools

import jax
import jax.numpy as jnp
from jax import lax
from jax.experimental import pallas as pl
from jax.experimental.pallas import tpu as pltpu
from jax.sharding import PartitionSpec as P

ONE_HOT = 256
GROUP = 8
VMEM_LIMIT = 32 * 1024 * 1024


def forward_kernel(rows, live, tid, bid, vol, tiles, out, vox, picked):
    angles, slots = tid.shape
    tile = tiles.shape[1]
    lines, width = vol.shape
    runs = width // tile
    step = 8
    for run in range(runs):
        for line in range(0, lines, step):
            vox[pl.ds(line * runs + run, step, stride=runs), :] = vol[
                line : line + step, run * tile : (run + 1) * tile
            ]

    def gather_angle(a, carry):
        def pair(i, inner):
            for u in range(2):
                k = i * 2 + u
                base = (a * slots + k) * rows
                for r in range(rows):
                    picked[pl.ds(base + r, 1), :] = vox[pl.ds(bid[a, k * rows + r], 1), :]
            return inner

        return lax.fori_loop(0, (live[a] + 1) // 2, pair, carry)

    lax.fori_loop(0, angles, gather_angle, 0)

    def project_angle(a, carry):
        count = live[a]

        def group(g, total):
            left, right = [], []
            for u in range(GROUP):
                k = g * GROUP + u
                part = picked[pl.ds(pl.multiple_of((a * slots + k) * rows, 8), rows), :]
                left.append(jnp.where(k < count, part, 0.0).astype(jnp.bfloat16))
                right.append(tiles[tid[a, k]])
            return total + lax.dot_general(
                jnp.concatenate(left, axis=1),
                jnp.concatenate(right, axis=1),
                (((1,), (1,)), ((), ())),
                preferred_element_type=jnp.float32,
            )

        total = lax.fori_loop(
            0, (count + GROUP - 1) // GROUP, group, jnp.zeros((rows, tile), jnp.float32)
        )
        out[pl.ds(pl.multiple_of(a * rows, 8), rows), :] = total
        return carry

    lax.fori_loop(0, angles, project_angle, 0)


def index_kernel(rows, runs, live, bid, hot, code):
    angles, length = bid.shape
    tile = code.shape[1]
    place = lax.broadcasted_iota(jnp.int32, (ONE_HOT, length), 0)
    position = lax.broadcasted_iota(jnp.int32, (1, length), 1)
    for a in range(angles):
        block = bid[a : a + 1, :]
        line = block // runs
        hot[a] = jnp.where(place == line % ONE_HOT, 1.0, 0.0).astype(jnp.bfloat16)
        group = (line // ONE_HOT) * runs + block % runs
        group = jnp.where(position < live[a] * rows, group, -1).astype(jnp.float32)
        for c in range(length // tile):
            wide = jnp.broadcast_to(group[:, c * tile : (c + 1) * tile], (tile, tile))
            code[a * length + c * tile : a * length + (c + 1) * tile, :] = wide.T.astype(
                jnp.bfloat16
            )


def backward_kernel(
    rows, live, tid, base, up, down, weight, tiles, hot, code, vol, col, out, res, spread, total
):
    angles, slots = tid.shape
    tile = tiles.shape[1]
    lines, width = vol.shape
    runs = width // tile
    rim = up.shape[0] // angles
    length = slots * rows
    for a in range(angles):
        own = base[a * rows : (a + 1) * rows, :]
        whole = jnp.concatenate(
            [
                own[:rim] + up[a * rim : (a + 1) * rim, :],
                own[rim : rows - rim],
                own[rows - rim :] + down[a * rim : (a + 1) * rim, :],
            ],
            axis=0,
        )
        res[a] = (weight[a * rows : (a + 1) * rows, :] * whole).astype(jnp.bfloat16)

    def spread_angle(a, carry):
        values = res[a]

        def group(g, inner):
            for u in range(0, GROUP, 2):
                k = g * GROUP + u
                pair = jnp.concatenate([tiles[tid[a, k]], tiles[tid[a, k + 1]]], axis=1)
                made = jnp.dot(values, pair, preferred_element_type=jnp.float32)
                both = jnp.concatenate([made[:, :tile], made[:, tile:]], axis=0)
                at = pl.multiple_of((a * slots + k) * rows, 16)
                spread[pl.ds(at, 2 * rows), :] = both.astype(jnp.bfloat16)
            return inner

        return lax.fori_loop(0, (live[a] + GROUP - 1) // GROUP, group, carry)

    lax.fori_loop(0, angles, spread_angle, 0)

    for chunk in range(lines // ONE_HOT):

        def add_angle(a, carry):
            at = pl.multiple_of(a * length, 128)
            values = spread[pl.ds(at, length), :]
            groups = code[pl.ds(at, length), :]
            right = jnp.concatenate(
                [
                    jnp.where(groups == jnp.bfloat16(chunk * runs + run), values, jnp.bfloat16(0))
                    for run in range(runs)
                ],
                axis=1,
            )
            made = jnp.dot(hot[a], right, preferred_element_type=jnp.float32)

            @pl.when(a == 0)
            def _():
                total[...] = made

            @pl.when(a > 0)
            def _():
                total[...] += made

            return carry

        lax.fori_loop(0, angles, add_angle, 0)
        here = slice(chunk * ONE_HOT, (chunk + 1) * ONE_HOT)
        out[here, :] = vol[here, :] + col[here, :] * total[...]


def swap(values, axis, bit):
    return lax.ppermute(values, axis, [(i, i ^ bit) for i in range(lax.axis_size(axis))])


def bits(axis):
    return [1 << i for i in range((lax.axis_size(axis) - 1).bit_length())]


def windows(data, slab_count, slab_depth, edge):
    padded = jnp.pad(data, ((0, 0), (1, 1), (0, 0)))
    parts = []
    for s in range(slab_count):
        part = padded[:, s * slab_depth : s * slab_depth + slab_depth + 2]
        if not edge:
            part = jnp.pad(part[:, 1:-1], ((0, 0), (1, 1), (0, 0)))
        parts.append(part)
    return jnp.stack(parts)


def on_device(volume, tile_table, tile_ids, block_ids, live_slots, measured, row_norm, col_norm):
    slab_depth, column_width, half_width = volume.shape
    tile_count, tile_size = (tile_table.shape[0], tile_table.shape[1])
    angle_count, slot_count = tile_ids.shape[3:]
    window = slab_depth + 2
    block_cols = block_ids.shape[4] // (slot_count * window)
    rows = window * block_cols
    rim = 2 * block_cols
    length = slot_count * rows
    lines = slab_depth * column_width
    runs = half_width // tile_size
    slab_count = lax.axis_size("gz")
    own_angles, local_cols = (measured.shape[0], measured.shape[1])

    tid = tile_ids.reshape(angle_count, slot_count)
    bid = block_ids.reshape(angle_count, length)
    live = live_slots.reshape(angle_count)
    vol = volume.reshape(lines, half_width)
    col = col_norm.reshape(lines, half_width)

    smem = pl.BlockSpec(memory_space=pltpu.SMEM)
    vmem = pl.BlockSpec(memory_space=pltpu.VMEM)
    params = pltpu.CompilerParams(vmem_limit_bytes=VMEM_LIMIT)

    me_z = lax.axis_index("gz")
    sends = jnp.concatenate(
        [
            windows(measured.transpose(0, 2, 1), slab_count, slab_depth, False),
            windows(row_norm.transpose(0, 2, 1), slab_count, slab_depth, True),
        ],
        axis=2,
    )
    got = [lax.dynamic_index_in_dim(sends, me_z, 0, False)]
    for step in range(1, slab_count):
        got.append(swap(lax.dynamic_index_in_dim(sends, me_z ^ step, 0, False), "gz", step))
    got = jnp.stack(got)
    arrived = jnp.concatenate(
        [lax.dynamic_index_in_dim(got, me_z ^ i, 0, False) for i in range(slab_count)], axis=0
    )
    target = arrived[:, :window]
    weight = arrived[:, window:][None]

    partial = pl.pallas_call(
        functools.partial(forward_kernel, rows),
        out_shape=jax.ShapeDtypeStruct((angle_count * rows, tile_size), jnp.float32),
        in_specs=[smem, smem, smem, vmem, vmem],
        out_specs=vmem,
        scratch_shapes=[
            pltpu.VMEM((lines * runs, tile_size), jnp.float32),
            pltpu.VMEM((angle_count * length, tile_size), jnp.float32),
        ],
        compiler_params=params,
        name="forward",
    )(live, tid, bid, vol, tile_table)

    hot, code = pl.pallas_call(
        functools.partial(index_kernel, rows, runs),
        out_shape=(
            jax.ShapeDtypeStruct((angle_count, ONE_HOT, length), jnp.bfloat16),
            jax.ShapeDtypeStruct((angle_count * length, tile_size), jnp.bfloat16),
        ),
        in_specs=[smem, vmem],
        out_specs=(vmem, vmem),
        compiler_params=params,
        name="index",
    )(live, bid)

    place = lax.axis_index("gx") * lax.axis_size("row") + lax.axis_index("row")
    if local_cols == tile_size:
        mine = lax.broadcasted_iota(jnp.int32, (1, 1, block_cols, 1), 2) == place
        spot = jnp.where(mine, target[:, :, None, :], 0.0)
    else:
        spot = jnp.zeros((angle_count, window, block_cols * tile_size), jnp.float32)
        spot = lax.dynamic_update_slice_in_dim(spot, target, place * local_cols, 2)
        spot = spot.reshape(angle_count, window, block_cols, tile_size)
    total = spot.reshape(angle_count * rows, tile_size) - partial
    for axis in ("row", "gx"):
        here = lax.axis_index(axis)
        for bit in bits(axis):
            other = swap(total, axis, bit)
            other_weight = swap(weight, axis, bit)
            total = total + other
            high = (here & bit) != 0
            weight = jnp.concatenate(
                [jnp.where(high, other_weight, weight), jnp.where(high, weight, other_weight)],
                axis=0,
            )
    weight = weight.transpose(1, 2, 0, 3).reshape(angle_count * rows, tile_size)
    blocks = total.reshape(angle_count, rows, tile_size)
    head = blocks[:, :rim].reshape(angle_count * rim, tile_size)
    tail = blocks[:, rows - rim :].reshape(angle_count * rim, tile_size)
    odd = (me_z & 1) == 1
    first = [(i, i ^ 1) for i in range(slab_count)]
    second = [(i, ((i + 1) ^ 1) - 1) for i in range(1, slab_count - 1)]
    one = lax.ppermute(jnp.where(odd, head, tail), "gz", first)
    two = lax.ppermute(jnp.where(odd, tail, head), "gz", second)
    up = jnp.where(odd, one, two)
    down = jnp.where(odd, two, one)

    made = pl.pallas_call(
        functools.partial(backward_kernel, rows),
        out_shape=jax.ShapeDtypeStruct((lines, half_width), jnp.float32),
        in_specs=[smem, smem] + [vmem] * 9,
        out_specs=vmem,
        scratch_shapes=[
            pltpu.VMEM((angle_count, rows, tile_size), jnp.bfloat16),
            pltpu.VMEM((angle_count * length, tile_size), jnp.bfloat16),
            pltpu.VMEM((ONE_HOT, half_width), jnp.float32),
        ],
        compiler_params=params,
        name="backward",
    )(live, tid, total, up, down, weight, tile_table, hot, code, vol, col)
    return made.reshape(slab_depth, column_width, half_width)


def solution(mesh):
    placed = (
        P(("grp", "gz"), "gx", "row"),
        P(),
        P("gz", "gx", "row", None, None),
        P("gz", "gx", "row", None, None),
        P("gz", "gx", "row", None),
        P(("grp", "gz"), ("gx", "row"), None),
        P("gz", ("gx", "row"), None),
        P("gz", "gx", "row"),
    )
    return jax.shard_map(
        on_device,
        mesh=mesh,
        in_specs=placed,
        out_specs=P(("grp", "gz"), "gx", "row"),
        check_vma=False,
    )
```

```python
import functools
import math

import jax
import jax.numpy as jnp
from jax import lax
from jax.experimental import pallas as pl
from jax.experimental.pallas import tpu as pltpu
from jax.sharding import PartitionSpec as P

ONE_HOT = 512
GROUP = 8
VMEM_LIMIT = 16 * 1024 * 1024


def forward_kernel(
    rows, live_in, tid_in, bid_in, vol_in, tiles_in, out,
    live, tid, bid, vol, tiles, vox, picked, sems,
):
    angles, slots = tid.shape
    tile = tiles.shape[1]
    lines, width = vol.shape
    runs = width // tile
    pairs = ((bid_in, bid), (tid_in, tid), (live_in, live), (vol_in, vol), (tiles_in, tiles))
    copies = [pltpu.make_async_copy(a, b, sems.at[i]) for i, (a, b) in enumerate(pairs)]
    for copy in copies:
        copy.start()
    copies[3].wait()
    step = 8
    for run in range(runs):
        for line in range(0, lines, step):
            vox[pl.ds(line * runs + run, step, stride=runs), :] = vol[
                line : line + step, run * tile : (run + 1) * tile
            ]
    for copy in copies[:3] + copies[4:]:
        copy.wait()

    def project_angle(a, carry):
        count = live[a]
        total = jnp.zeros((rows, tile), jnp.float32)
        for g in range(0, slots, GROUP):
            left, right = [], []
            for k in range(g, g + GROUP):
                for r in range(rows):
                    j = k * rows + r
                    picked[j : j + 1, :] = vox[pl.ds(bid[a, j], 1), :]
            for k in range(g, g + GROUP):
                part = picked[k * rows : (k + 1) * rows, :]
                left.append(jnp.where(k < count, part, 0.0).astype(jnp.bfloat16))
                right.append(tiles[tid[a, k]])
            total += lax.dot_general(
                jnp.concatenate(left, axis=1),
                jnp.concatenate(right, axis=1),
                (((1,), (1,)), ((), ())),
                preferred_element_type=jnp.float32,
            )
        out[pl.ds(pl.multiple_of(a * rows, 8), rows), :] = total
        return carry

    lax.fori_loop(0, angles, project_angle, 0)


def index_kernel(rows, runs, live, bid, hot, code):
    angles, length = bid.shape
    tile = code.shape[1]
    high = hot.shape[0]
    place = lax.broadcasted_iota(jnp.int32, (high, length), 0)
    position = lax.broadcasted_iota(jnp.int32, (1, length), 1)
    for a in range(angles):
        block = bid[a : a + 1, :]
        line = block // runs
        hot[:, a * length : (a + 1) * length] = jnp.where(
            place == line % high, 1.0, 0.0
        ).astype(jnp.bfloat16)
        group = (line // high) * runs + block % runs
        group = jnp.where(position < live[a] * rows, group, -1).astype(jnp.float32)
        for c in range(length // tile):
            wide = jnp.broadcast_to(group[:, c * tile : (c + 1) * tile], (tile, tile))
            code[a * length + c * tile : a * length + (c + 1) * tile, :] = wide.T.astype(
                jnp.bfloat16
            )


def backward_kernel(
    rows, live, tid, base, up, down, weight, tiles, hot, code, vol_in, col_in, out_in,
    res, spread, vol, col, out, sems,
):
    angles, slots = tid.shape
    tile = tiles.shape[1]
    lines, width = vol.shape
    runs = width // tile
    rim = up.shape[0] // angles
    high = hot.shape[0]
    reads = [
        pltpu.make_async_copy(vol_in, vol, sems.at[0]),
        pltpu.make_async_copy(col_in, col, sems.at[1]),
    ]
    for copy in reads:
        copy.start()
    for a in range(angles):
        own = base[a * rows : (a + 1) * rows, :]
        whole = jnp.concatenate(
            [
                own[:rim] + up[a * rim : (a + 1) * rim, :],
                own[rim : rows - rim],
                own[rows - rim :] + down[a * rim : (a + 1) * rim, :],
            ],
            axis=0,
        )
        res[a] = (weight[a * rows : (a + 1) * rows, :] * whole).astype(jnp.bfloat16)

    def spread_angle(a, carry):
        values = res[a]

        def group(g, inner):
            for u in range(0, GROUP, 2):
                k = g * GROUP + u
                pair = jnp.concatenate([tiles[tid[a, k]], tiles[tid[a, k + 1]]], axis=1)
                made = jnp.dot(values, pair, preferred_element_type=jnp.float32)
                both = jnp.concatenate([made[:, :tile], made[:, tile:]], axis=0)
                at = pl.multiple_of((a * slots + k) * rows, 16)
                spread[pl.ds(at, 2 * rows), :] = both.astype(jnp.bfloat16)
            return inner

        return lax.fori_loop(0, (live[a] + GROUP - 1) // GROUP, group, carry)

    lax.fori_loop(0, angles, spread_angle, 0)
    for copy in reads:
        copy.wait()

    writes = []
    for chunk in range(lines // high):
        values = spread[...]
        groups = code[...]
        right = jnp.concatenate(
            [
                jnp.where(groups == jnp.bfloat16(chunk * runs + run), values, jnp.bfloat16(0))
                for run in range(runs)
            ],
            axis=1,
        )
        made = jnp.dot(hot[...], right, preferred_element_type=jnp.float32)
        here = pl.ds(chunk * high, high)
        out[here, :] = vol[here, :] + col[here, :] * made
        copy = pltpu.make_async_copy(out.at[here, :], out_in.at[here, :], sems.at[2 + chunk])
        copy.start()
        writes.append(copy)
    for copy in writes:
        copy.wait()


def swap(values, axis, bit):
    return lax.ppermute(values, axis, [(i, i ^ bit) for i in range(lax.axis_size(axis))])


def bits(axis):
    return [1 << i for i in range((lax.axis_size(axis) - 1).bit_length())]


def windows(data, slab_count, slab_depth, edge):
    padded = jnp.pad(data, ((0, 0), (1, 1), (0, 0)))
    parts = []
    for s in range(slab_count):
        part = padded[:, s * slab_depth : s * slab_depth + slab_depth + 2]
        if not edge:
            part = jnp.pad(part[:, 1:-1], ((0, 0), (1, 1), (0, 0)))
        parts.append(part)
    return jnp.stack(parts)


def ordered(mine_high, own, other, axis):
    return jnp.concatenate(
        [jnp.where(mine_high, other, own), jnp.where(mine_high, own, other)], axis=axis
    )


def to_slabs(sends):
    here = lax.axis_index("gz")
    for bit in bits("gz"):
        high = (here & bit) != 0
        halves = sends.reshape((sends.shape[0] // 2, 2) + sends.shape[1:])
        keep = jnp.where(high, halves[:, 1], halves[:, 0])
        give = jnp.where(high, halves[:, 0], halves[:, 1])
        sends = ordered(high, keep, swap(give, "gz", bit), 1)
    return sends[0]


def on_device(volume, tile_table, tile_ids, block_ids, live_slots, measured, row_norm, col_norm):
    slab_depth, column_width, half_width = volume.shape
    tile_size = tile_table.shape[1]
    angle_count, slot_count = tile_ids.shape[3:]
    window = slab_depth + 2
    block_cols = block_ids.shape[4] // (slot_count * window)
    rows = window * block_cols
    rim = 2 * block_cols
    length = slot_count * rows
    lines = slab_depth * column_width
    runs = half_width // tile_size
    high = math.gcd(lines, ONE_HOT)
    slab_count = lax.axis_size("gz")
    local_cols = measured.shape[1]

    tid = tile_ids.reshape(angle_count, slot_count)
    bid = block_ids.reshape(angle_count, length)
    live = live_slots.reshape(angle_count)
    vol = volume.reshape(lines, half_width)
    col = col_norm.reshape(lines, half_width)

    smem = pl.BlockSpec(memory_space=pltpu.SMEM)
    vmem = pl.BlockSpec(memory_space=pltpu.VMEM)
    hbm = pl.BlockSpec(memory_space=pltpu.HBM)
    params = pltpu.CompilerParams(vmem_limit_bytes=VMEM_LIMIT)

    arrived = to_slabs(
        jnp.concatenate(
            [
                windows(measured.transpose(0, 2, 1), slab_count, slab_depth, False),
                windows(row_norm.transpose(0, 2, 1), slab_count, slab_depth, True),
            ],
            axis=2,
        )
    )
    target = arrived[:, :window]
    weight = arrived[:, window:].reshape(angle_count * window, local_cols)[None]

    partial = pl.pallas_call(
        functools.partial(forward_kernel, rows),
        out_shape=jax.ShapeDtypeStruct((angle_count * rows, tile_size), jnp.float32),
        in_specs=[hbm] * 5,
        out_specs=vmem,
        scratch_shapes=[
            pltpu.SMEM((angle_count,), jnp.int32),
            pltpu.SMEM((angle_count, slot_count), jnp.int32),
            pltpu.SMEM((angle_count, length), jnp.int32),
            pltpu.VMEM((lines, half_width), jnp.float32),
            pltpu.VMEM(tile_table.shape, jnp.bfloat16),
            pltpu.VMEM((lines * runs, tile_size), jnp.float32),
            pltpu.VMEM((length, tile_size), jnp.float32),
            pltpu.SemaphoreType.DMA((5,)),
        ],
        compiler_params=params,
        name="forward",
    )(live, tid, bid, vol, tile_table)

    hot, code = pl.pallas_call(
        functools.partial(index_kernel, rows, runs),
        out_shape=(
            jax.ShapeDtypeStruct((high, angle_count * length), jnp.bfloat16),
            jax.ShapeDtypeStruct((angle_count * length, tile_size), jnp.bfloat16),
        ),
        in_specs=[smem, vmem],
        out_specs=(vmem, vmem),
        compiler_params=params,
        name="index",
    )(live, bid)

    row_count = lax.axis_size("row")
    at_row = lax.axis_index("row")
    place = lax.axis_index("gx") * row_count + at_row
    if local_cols == tile_size:
        mine = lax.broadcasted_iota(jnp.int32, (1, 1, block_cols, 1), 2) == place
        spot = jnp.where(mine, target[:, :, None, :], 0.0)
    else:
        spot = jnp.zeros((angle_count, window, block_cols * tile_size), jnp.float32)
        spot = lax.dynamic_update_slice_in_dim(spot, target, place * local_cols, 2)
        spot = spot.reshape(angle_count, window, block_cols, tile_size)
    total = spot.reshape(angle_count * rows, tile_size) - partial
    for bit in bits("row"):
        total = total + swap(total, "row", bit)
    for bit in bits("gx"):
        is_high = (lax.axis_index("gx") & bit) != 0
        if local_cols == tile_size:
            both = jnp.concatenate([total, weight.reshape(-1, tile_size)], axis=0)
            came = swap(both, "gx", bit)
            other_weight = came[total.shape[0] :].reshape(weight.shape)
            came = came[: total.shape[0]]
        else:
            came = swap(total, "gx", bit)
            other_weight = swap(weight, "gx", bit)
        total = total + came
        weight = ordered(is_high, weight, other_weight, 0)

    blocks = total.reshape(angle_count, rows, tile_size)
    head = blocks[:, :rim].reshape(angle_count * rim, tile_size)
    tail = blocks[:, rows - rim :].reshape(angle_count * rim, tile_size)
    last = slab_count - 1
    assert row_count == 2
    upper = at_row == 1
    hops = [((z + 1) * 2, z * 2) for z in range(last)]
    hops += [(z * 2 + 1, z * 2 + 3) for z in range(last)]
    came = lax.ppermute(jnp.where(upper, tail, head), ("gz", "row"), hops)
    if local_cols == tile_size:
        both = jnp.concatenate([came, weight.reshape(-1, tile_size)], axis=0)
        swapped = swap(both, "row", 1)
        other_came = swapped[: came.shape[0]]
        other_weight = swapped[came.shape[0] :].reshape(weight.shape)
    else:
        other_came = swap(came, "row", 1)
        other_weight = swap(weight, "row", 1)
    up = jnp.where(upper, came, other_came)
    down = jnp.where(upper, other_came, came)
    weight = ordered(upper, weight[:, None], other_weight[:, None], 1)
    weight = weight.reshape(-1, angle_count, window, local_cols)
    weight = weight.transpose(1, 2, 0, 3).reshape(angle_count * rows, tile_size)

    made = pl.pallas_call(
        functools.partial(backward_kernel, rows),
        out_shape=jax.ShapeDtypeStruct((lines, half_width), jnp.float32),
        in_specs=[smem, smem] + [vmem] * 7 + [hbm] * 2,
        out_specs=hbm,
        scratch_shapes=[
            pltpu.VMEM((angle_count, rows, tile_size), jnp.bfloat16),
            pltpu.VMEM((angle_count * length, tile_size), jnp.bfloat16),
            pltpu.VMEM((lines, half_width), jnp.float32),
            pltpu.VMEM((lines, half_width), jnp.float32),
            pltpu.VMEM((lines, half_width), jnp.float32),
            pltpu.SemaphoreType.DMA((2 + lines // high,)),
        ],
        compiler_params=params,
        name="backward",
    )(live, tid, total, up, down, weight, tile_table, hot, code, vol, col)
    return made.reshape(slab_depth, column_width, half_width)


def solution(mesh):
    placed = (
        P(("grp", "gz"), "gx", "row"),
        P(),
        P("gz", "gx", "row", None, None),
        P("gz", "gx", "row", None, None),
        P("gz", "gx", "row", None),
        P(("grp", "gz"), ("gx", "row"), None),
        P("gz", ("gx", "row"), None),
        P("gz", "gx", "row"),
    )
    return jax.shard_map(
        on_device,
        mesh=mesh,
        in_specs=placed,
        out_specs=P(("grp", "gz"), "gx", "row"),
        check_vma=False,
    )
```

```python
import functools
import math

import jax
import jax.numpy as jnp
from jax import lax
from jax.experimental import pallas as pl
from jax.experimental.pallas import tpu as pltpu
from jax.sharding import PartitionSpec as P

ONE_HOT = 256
GROUP = 8
STATIC_ROWS = 4096
VMEM_LIMIT = 16 * 1024 * 1024


def forward_kernel(
    rows, window, live_in, tid_in, bid_in, vol_in, tiles_in, target_in, weight_in, out, sends,
    live, tid, bid, vol, tiles, target, weight, vox, picked, sems,
):
    angles, slots = tid.shape
    tile = tiles.shape[1]
    lines, width = vol.shape
    runs = width // tile
    pairs = (
        (bid_in, bid), (live_in, live), (tid_in, tid), (vol_in, vol),
        (target_in, target), (weight_in, weight), (tiles_in, tiles),
    )
    copies = [pltpu.make_async_copy(a, b, sems.at[i]) for i, (a, b) in enumerate(pairs)]
    for copy in copies:
        copy.start()
    copies[3].wait()
    step = 8
    for run in range(runs):
        for line in range(0, lines, step):
            vox[pl.ds(line * runs + run, step, stride=runs), :] = vol[
                line : line + step, run * tile : (run + 1) * tile
            ]
    for copy in copies[:3] + copies[4:6]:
        copy.wait()
    slabs = sends.shape[0]
    depth = window - 2
    sends[...] = jnp.zeros_like(sends)
    for s in range(slabs):
        low, high = max(s * depth - 1, 0), min(s * depth + depth + 1, slabs * depth)
        skip = low - (s * depth - 1)
        for own in range(target.shape[0]):
            for at, data in ((0, target), (window, weight)):
                sends[s, own, at + skip : at + skip + high - low, :] = data[own, low:high, :]

    def gather(a, at):
        for j in range(slots * rows):
            picked[at + j : at + j + 1, :] = vox[pl.ds(bid[a, j], 1), :]

    def project(a, at):
        count = live[a]
        total = jnp.zeros((rows, tile), jnp.float32)
        for g in range(0, slots, GROUP):
            left, right = [], []
            for k in range(g, g + GROUP):
                part = picked[at + k * rows : at + (k + 1) * rows, :]
                left.append(jnp.where(k < count, part, 0.0).astype(jnp.bfloat16))
                right.append(tiles[tid[a, k]])
            total += lax.dot_general(
                jnp.concatenate(left, axis=1),
                jnp.concatenate(right, axis=1),
                (((1,), (1,)), ((), ())),
                preferred_element_type=jnp.float32,
            )
        return total

    length = slots * rows
    if angles * length <= STATIC_ROWS:
        gather(0, 0)
        copies[6].wait()
        for a in range(angles):

            @pl.when(live[a] >= 0)
            def _():
                if a + 1 < angles:
                    gather(a + 1, (a + 1) % 2 * length)
                out[a * rows : (a + 1) * rows, :] = project(a, a % 2 * length)

    else:
        copies[6].wait()

        def project_angle(a, carry):
            gather(a, 0)
            out[pl.ds(pl.multiple_of(a * rows, 8), rows), :] = project(a, 0)
            return carry

        lax.fori_loop(0, angles, project_angle, 0)


def backward_kernel(
    rows, live, tid, bid, head, middle, tail, target, weight, tiles, vol_in, col_in, out_in,
    res, hot, code, spread, vol, col, out, sems,
):
    angles, slots = tid.shape
    tile = tiles.shape[1]
    lines, width = vol.shape
    runs = width // tile
    high = hot.shape[0]
    length = slots * rows
    reads = [
        pltpu.make_async_copy(vol_in, vol, sems.at[0]),
        pltpu.make_async_copy(col_in, col, sems.at[1]),
    ]
    for copy in reads:
        copy.start()
    for a in range(angles):
        parts = []
        for part in (head, middle, tail):
            size = part.shape[0] // angles
            parts.append(part[a * size : (a + 1) * size, :])
        here = slice(a * rows, (a + 1) * rows)
        error = target[here, :] - jnp.concatenate(parts, axis=0)
        res[a] = (weight[here, :] * error).astype(jnp.bfloat16)

    place = lax.broadcasted_iota(jnp.int32, (high, tile), 0)
    position = lax.broadcasted_iota(jnp.int32, (1, tile), 1)
    for a in range(angles):
        groups = []
        for c in range(0, length, tile):
            block = bid[a : a + 1, c : c + tile]
            line = block // runs
            hot[:, a * length + c : a * length + c + tile] = jnp.where(
                place == line % high, 1.0, 0.0
            ).astype(jnp.bfloat16)
            group = (line // high) * runs + block % runs
            groups.append(jnp.where(position + c < live[a] * rows, group, -1))
        pad = -len(groups) % 8
        groups += [jnp.zeros((1, tile), jnp.int32)] * pad
        turned = jnp.concatenate(groups, axis=0).astype(jnp.float32).T
        for i in range(length // tile):
            wide = jnp.broadcast_to(turned[:, i : i + 1], (tile, tile))
            code[a * length + i * tile : a * length + (i + 1) * tile, :] = wide.astype(
                jnp.bfloat16
            )

    def spread_angle(a, carry):
        values = res[a]

        def group(g, inner):
            for u in range(0, GROUP, 2):
                k = g * GROUP + u
                pair = jnp.concatenate([tiles[tid[a, k]], tiles[tid[a, k + 1]]], axis=1)
                made = jnp.dot(values, pair, preferred_element_type=jnp.float32)
                both = jnp.concatenate([made[:, :tile], made[:, tile:]], axis=0)
                at = pl.multiple_of((a * slots + k) * rows, 16)
                spread[pl.ds(at, 2 * rows), :] = both.astype(jnp.bfloat16)
            return inner

        return lax.fori_loop(0, (live[a] + GROUP - 1) // GROUP, group, carry)

    lax.fori_loop(0, angles, spread_angle, 0)

    writes = []
    for chunk in range(lines // high):
        values = spread[...]
        groups = code[...]
        right = jnp.concatenate(
            [
                jnp.where(groups == jnp.bfloat16(chunk * runs + run), values, jnp.bfloat16(0))
                for run in range(runs)
            ],
            axis=1,
        )
        made = jnp.dot(hot[...], right, preferred_element_type=jnp.float32)
        if chunk == 0:
            for copy in reads:
                copy.wait()
        here = pl.ds(chunk * high, high)
        out[here, :] = vol[here, :] + col[here, :] * made
        copy = pltpu.make_async_copy(out.at[here, :], out_in.at[here, :], sems.at[2 + chunk])
        copy.start()
        writes.append(copy)
    for copy in writes:
        copy.wait()


def swap(values, axis, bit):
    return lax.ppermute(values, axis, [(i, i ^ bit) for i in range(lax.axis_size(axis))])


def swap_many(arrays, axis, bit):
    if len({array.shape[-1] for array in arrays}) > 1:
        return [swap(array, axis, bit) for array in arrays]
    width = arrays[0].shape[-1]
    came = swap(jnp.concatenate([a.reshape(-1, width) for a in arrays], axis=0), axis, bit)
    out, at = [], 0
    for array in arrays:
        count = array.size // width
        out.append(came[at : at + count].reshape(array.shape))
        at += count
    return out


def bits(axis):
    return [1 << i for i in range((lax.axis_size(axis) - 1).bit_length())]


def ordered(mine_high, own, other, axis):
    return jnp.concatenate(
        [jnp.where(mine_high, other, own), jnp.where(mine_high, own, other)], axis=axis
    )


def to_slabs(sends, anchors):
    here = lax.axis_index("gz")
    for bit in bits("gz"):
        high = (here & bit) != 0
        halves = sends.reshape((sends.shape[0] // 2, 2) + sends.shape[1:])
        keep = jnp.where(high, halves[:, 1], halves[:, 0])
        give = jnp.where(high, halves[:, 0], halves[:, 1])
        came = swap(give, "gz", bit)
        if bit in anchors:
            came, _ = lax.optimization_barrier((came, anchors[bit]))
        sends = ordered(high, keep, came, 1)
    return sends[0]


def on_device(volume, tile_table, tile_ids, block_ids, live_slots, measured, row_norm, col_norm):
    slab_depth, column_width, half_width = volume.shape
    tile_size = tile_table.shape[1]
    angle_count, slot_count = tile_ids.shape[3:]
    window = slab_depth + 2
    block_cols = block_ids.shape[4] // (slot_count * window)
    rows = window * block_cols
    rim = 2 * block_cols
    length = slot_count * rows
    lines = slab_depth * column_width
    runs = half_width // tile_size
    high = math.gcd(lines, ONE_HOT)
    slab_count = lax.axis_size("gz")
    own_angles, local_cols, row_total = measured.shape

    def held(array):
        return pltpu.with_memory_space_constraint(array, pltpu.HBM)

    tid = tile_ids.reshape(angle_count, slot_count)
    bid = block_ids.reshape(angle_count, length)
    live = live_slots.reshape(angle_count)
    vol = held(volume.reshape(lines, half_width))
    col = held(col_norm.reshape(lines, half_width))

    smem = pl.BlockSpec(memory_space=pltpu.SMEM)
    vmem = pl.BlockSpec(memory_space=pltpu.VMEM)
    hbm = pl.BlockSpec(memory_space=pltpu.HBM)
    params = pltpu.CompilerParams(vmem_limit_bytes=VMEM_LIMIT)
    buffers = 2 if angle_count * length <= STATIC_ROWS else 1

    partial, sends = pl.pallas_call(
        functools.partial(forward_kernel, rows, window),
        out_shape=(
            jax.ShapeDtypeStruct((angle_count * rows, tile_size), jnp.float32),
            jax.ShapeDtypeStruct((slab_count, own_angles, 2 * window, local_cols), jnp.float32),
        ),
        in_specs=[hbm] * 7,
        out_specs=(vmem, vmem),
        scratch_shapes=[
            pltpu.SMEM((angle_count,), jnp.int32),
            pltpu.SMEM((angle_count, slot_count), jnp.int32),
            pltpu.SMEM((angle_count, length), jnp.int32),
            pltpu.VMEM((lines, half_width), jnp.float32),
            pltpu.VMEM(tile_table.shape, jnp.bfloat16),
            pltpu.VMEM((own_angles, row_total, local_cols), jnp.float32),
            pltpu.VMEM((own_angles, row_total, local_cols), jnp.float32),
            pltpu.VMEM((lines * runs, tile_size), jnp.float32),
            pltpu.VMEM((buffers * length, tile_size), jnp.float32),
            pltpu.SemaphoreType.DMA((7,)),
        ],
        compiler_params=params,
        name="forward",
    )(
        held(live), held(tid), held(bid), vol, held(tile_table),
        held(measured.transpose(0, 2, 1)), held(row_norm.transpose(0, 2, 1)),
    )

    assert lax.axis_size("row") == 2
    upper = lax.axis_index("row") == 1
    total = partial + swap(partial, "row", 1)
    blocks = total.reshape(angle_count, rows, tile_size)
    outer = jnp.where(upper, blocks[:, rows - rim :], blocks[:, :rim])
    middle = blocks[:, rim : rows - rim]
    for bit in bits("gx"):
        came = swap_many([outer, middle], "gx", bit)
        outer, middle = outer + came[0], middle + came[1]
    last = slab_count - 1
    hops = [((z + 1) * 2, z * 2) for z in range(last)]
    hops += [(z * 2 + 1, z * 2 + 3) for z in range(last)]
    rims = lax.ppermute(outer.reshape(angle_count * rim, tile_size), ("gz", "row"), hops)
    outer = outer.reshape(rims.shape)

    columns = to_slabs(sends, {1: total, 2: outer})[None]
    for bit in bits("gx"):
        came = swap(columns, "gx", bit)
        columns = ordered((lax.axis_index("gx") & bit) != 0, columns, came, 0)
    other_outer, other_rims, other_columns = swap_many([outer, rims, columns], "row", 1)
    own_rim = outer + other_rims
    far_rim = other_outer + rims
    head = jnp.where(upper, far_rim, own_rim)
    tail = jnp.where(upper, own_rim, far_rim)
    columns = ordered(upper, columns[:, None], other_columns[:, None], 1)
    columns = columns.reshape(-1, angle_count, 2, window, local_cols)
    columns = columns.transpose(2, 1, 3, 0, 4).reshape(2, angle_count * rows, tile_size)

    made = pl.pallas_call(
        functools.partial(backward_kernel, rows),
        out_shape=jax.ShapeDtypeStruct((lines, half_width), jnp.float32),
        in_specs=[smem, smem] + [vmem] * 7 + [hbm] * 2,
        out_specs=hbm,
        scratch_shapes=[
            pltpu.VMEM((angle_count, rows, tile_size), jnp.bfloat16),
            pltpu.VMEM((high, angle_count * length), jnp.bfloat16),
            pltpu.VMEM((angle_count * length, tile_size), jnp.bfloat16),
            pltpu.VMEM((angle_count * length, tile_size), jnp.bfloat16),
            pltpu.VMEM((lines, half_width), jnp.float32),
            pltpu.VMEM((lines, half_width), jnp.float32),
            pltpu.VMEM((lines, half_width), jnp.float32),
            pltpu.SemaphoreType.DMA((2 + lines // high,)),
        ],
        compiler_params=params,
        name="backward",
    )(
        live, tid, bid, head, middle.reshape(-1, tile_size), tail, columns[0], columns[1],
        tile_table, vol, col,
    )
    return made.reshape(slab_depth, column_width, half_width)


def solution(mesh):
    placed = (
        P(("grp", "gz"), "gx", "row"),
        P(),
        P("gz", "gx", "row", None, None),
        P("gz", "gx", "row", None, None),
        P("gz", "gx", "row", None),
        P(("grp", "gz"), ("gx", "row"), None),
        P("gz", ("gx", "row"), None),
        P("gz", "gx", "row"),
    )

    return jax.shard_map(
        on_device,
        mesh=mesh,
        in_specs=placed,
        out_specs=P(("grp", "gz"), "gx", "row"),
        check_vma=False,
    )
```

```python
import functools
import math

import jax
import jax.numpy as jnp
from jax import lax
from jax.experimental import pallas as pl
from jax.experimental.pallas import tpu as pltpu
from jax.sharding import PartitionSpec as P

ONE_HOT = 256
GROUP = 8
STATIC_ROWS = 4096
VMEM_LIMIT = 16 * 1024 * 1024


def pack_kernel(window, target_in, weight_in, sends, target, weight, sems):
    copies = [
        pltpu.make_async_copy(target_in, target, sems.at[0]),
        pltpu.make_async_copy(weight_in, weight, sems.at[1]),
    ]
    for copy in copies:
        copy.start()
    sends[...] = jnp.zeros_like(sends)
    for copy in copies:
        copy.wait()
    slabs = sends.shape[0]
    depth = window - 2
    for s in range(slabs):
        low, high = max(s * depth - 1, 0), min(s * depth + depth + 1, slabs * depth)
        skip = low - (s * depth - 1)
        for own in range(target.shape[0]):
            for at, data in ((0, target), (window, weight)):
                sends[s, own, at + skip : at + skip + high - low, :] = data[own, low:high, :]


def forward_kernel(
    rows, live_in, tid_in, bid_in, vol_in, tiles_in, out,
    live, tid, bid, vol, tiles, vox, picked, sems,
):
    angles, slots = tid.shape
    tile = tiles.shape[1]
    lines, width = vol.shape
    runs = width // tile
    pairs = ((bid_in, bid), (live_in, live), (tid_in, tid), (vol_in, vol), (tiles_in, tiles))
    copies = [pltpu.make_async_copy(a, b, sems.at[i]) for i, (a, b) in enumerate(pairs)]
    for copy in copies:
        copy.start()
    copies[3].wait()
    step = 8
    for run in range(runs):
        for line in range(0, lines, step):
            vox[pl.ds(line * runs + run, step, stride=runs), :] = vol[
                line : line + step, run * tile : (run + 1) * tile
            ]
    for copy in copies[:3]:
        copy.wait()

    def gather(a, at):
        for j in range(slots * rows):
            picked[at + j : at + j + 1, :] = vox[pl.ds(bid[a, j], 1), :]

    def project(a, at):
        count = live[a]
        total = jnp.zeros((rows, tile), jnp.float32)
        for g in range(0, slots, GROUP):
            left, right = [], []
            for k in range(g, g + GROUP):
                part = picked[at + k * rows : at + (k + 1) * rows, :]
                left.append(jnp.where(k < count, part, 0.0).astype(jnp.bfloat16))
                right.append(tiles[tid[a, k]])
            total += lax.dot_general(
                jnp.concatenate(left, axis=1),
                jnp.concatenate(right, axis=1),
                (((1,), (1,)), ((), ())),
                preferred_element_type=jnp.float32,
            )
        return total

    length = slots * rows
    if angles * length <= STATIC_ROWS:
        gather(0, 0)
        copies[4].wait()
        for a in range(angles):

            @pl.when(live[a] >= 0)
            def _():
                if a + 1 < angles:
                    gather(a + 1, (a + 1) % 2 * length)
                out[a * rows : (a + 1) * rows, :] = project(a, a % 2 * length)

    else:
        copies[4].wait()

        def project_angle(a, carry):
            gather(a, 0)
            out[pl.ds(pl.multiple_of(a * rows, 8), rows), :] = project(a, 0)
            return carry

        lax.fori_loop(0, angles, project_angle, 0)


def backward_kernel(
    rows, live, tid, bid, head, middle, tail, target, weight, tiles, vol_in, col_in, out_in,
    res, hot, code, spread, vol, col, out, total, sems,
):
    angles, slots = tid.shape
    tile = tiles.shape[1]
    lines, width = vol.shape
    runs = width // tile
    high = hot.shape[0]
    length = slots * rows
    reads = [
        pltpu.make_async_copy(vol_in, vol, sems.at[0]),
        pltpu.make_async_copy(col_in, col, sems.at[1]),
    ]
    for copy in reads:
        copy.start()
    for a in range(angles):
        parts = []
        for part in (head, middle, tail):
            size = part.shape[0] // angles
            parts.append(part[a * size : (a + 1) * size, :])
        here = slice(a * rows, (a + 1) * rows)
        error = target[here, :] - jnp.concatenate(parts, axis=0)
        res[a] = (weight[here, :] * error).astype(jnp.bfloat16)

    place = lax.broadcasted_iota(jnp.int32, (high, tile), 0).astype(jnp.bfloat16)
    position = lax.broadcasted_iota(jnp.int32, (1, tile), 1)
    for a in range(angles):
        groups = []
        for c in range(0, length, tile):
            block = bid[a : a + 1, c : c + tile]
            line = block // runs
            low = (line % high).astype(jnp.bfloat16)
            hot[:, a * length + c : a * length + c + tile] = jnp.where(
                place == low, jnp.bfloat16(1), jnp.bfloat16(0)
            )
            group = (line // high) * runs + block % runs
            groups.append(jnp.where(position + c < live[a] * rows, group, -1))
        pad = -len(groups) % 8
        groups += [jnp.zeros((1, tile), jnp.int32)] * pad
        turned = jnp.concatenate(groups, axis=0).astype(jnp.float32).T
        for i in range(length // tile):
            wide = jnp.broadcast_to(turned[:, i : i + 1], (tile, tile))
            code[a * length + i * tile : a * length + (i + 1) * tile, :] = wide.astype(
                jnp.bfloat16
            )

    def spread_pair(values, a, k, at):
        pair = jnp.concatenate([tiles[tid[a, k]], tiles[tid[a, k + 1]]], axis=1)
        made = jnp.dot(values, pair, preferred_element_type=jnp.float32)
        both = jnp.concatenate([made[:, :tile], made[:, tile:]], axis=0)
        spread[pl.ds(at, 2 * rows), :] = both.astype(jnp.bfloat16)

    def add_part(at, size, first, count):
        values = spread[pl.ds(at, size), :]
        groups = code[pl.ds(at, size), :]
        right = jnp.concatenate(
            [
                jnp.where(groups == jnp.bfloat16(g), values, jnp.bfloat16(0))
                for g in range(first * runs, (first + count) * runs)
            ],
            axis=1,
        )
        return jnp.dot(hot[:, pl.ds(at, size)], right, preferred_element_type=jnp.float32)

    chunks = lines // high
    writes = []

    def finish(first, count, made):
        for i in range(count):
            here = pl.ds((first + i) * high, high)
            out[here, :] = vol[here, :] + col[here, :] * made[:, i * width : (i + 1) * width]
            copy = pltpu.make_async_copy(
                out.at[here, :], out_in.at[here, :], sems.at[2 + first + i]
            )
            copy.start()
            writes.append(copy)

    if angles * length <= STATIC_ROWS:
        for a in range(angles):
            values = res[a]
            for k in range(0, slots, 2):
                spread_pair(values, a, k, (a * slots + k) * rows)
        made = add_part(0, angles * length, 0, chunks)
        for copy in reads:
            copy.wait()
        finish(0, chunks, made)
    else:

        def step(a, carry):
            values = res[a]
            base = pl.multiple_of(a * length, 256)
            for k in range(0, slots, 2):
                spread_pair(values, a, k, base + k * rows)
            total[...] += add_part(base, length, 0, chunks)
            return carry

        total[...] = jnp.zeros_like(total)
        lax.fori_loop(0, angles, step, 0)
        for copy in reads:
            copy.wait()
        finish(0, chunks, total[...])
    for copy in writes:
        copy.wait()


def swap(values, axis, bit):
    return lax.ppermute(values, axis, [(i, i ^ bit) for i in range(lax.axis_size(axis))])


def swap_many(arrays, axis, bit):
    if len({array.shape[-1] for array in arrays}) > 1:
        return [swap(array, axis, bit) for array in arrays]
    width = arrays[0].shape[-1]
    came = swap(jnp.concatenate([a.reshape(-1, width) for a in arrays], axis=0), axis, bit)
    out, at = [], 0
    for array in arrays:
        count = array.size // width
        out.append(came[at : at + count].reshape(array.shape))
        at += count
    return out


def bits(axis):
    return [1 << i for i in range((lax.axis_size(axis) - 1).bit_length())]


def ordered(mine_high, own, other, axis):
    return jnp.concatenate(
        [jnp.where(mine_high, other, own), jnp.where(mine_high, own, other)], axis=axis
    )


def exchange_slabs(parts, bit):
    high = (lax.axis_index("gz") & bit) != 0
    count = parts.shape[0] // 2
    halves = parts.reshape((2, count) + parts.shape[1:])
    keep = jnp.where(high, halves[1], halves[0])
    give = jnp.where(high, halves[0], halves[1])
    came = swap(give, "gz", bit)
    low, up = jnp.where(high, came, keep), jnp.where(high, keep, came)
    both = jnp.stack([low, up], axis=2)
    return both.reshape((count, parts.shape[1] * 2) + parts.shape[2:])


def on_device(volume, tile_table, tile_ids, block_ids, live_slots, measured, row_norm, col_norm):
    slab_depth, column_width, half_width = volume.shape
    tile_size = tile_table.shape[1]
    angle_count, slot_count = tile_ids.shape[3:]
    window = slab_depth + 2
    block_cols = block_ids.shape[4] // (slot_count * window)
    rows = window * block_cols
    rim = 2 * block_cols
    length = slot_count * rows
    lines = slab_depth * column_width
    runs = half_width // tile_size
    high = math.gcd(lines, ONE_HOT)
    slab_count = lax.axis_size("gz")
    own_angles, local_cols, row_total = measured.shape

    def held(array):
        return pltpu.with_memory_space_constraint(array, pltpu.HBM)

    tid = tile_ids.reshape(angle_count, slot_count)
    bid = block_ids.reshape(angle_count, length)
    live = live_slots.reshape(angle_count)
    vol = held(volume.reshape(lines, half_width))
    col = held(col_norm.reshape(lines, half_width))

    smem = pl.BlockSpec(memory_space=pltpu.SMEM)
    vmem = pl.BlockSpec(memory_space=pltpu.VMEM)
    hbm = pl.BlockSpec(memory_space=pltpu.HBM)
    params = pltpu.CompilerParams(vmem_limit_bytes=VMEM_LIMIT)
    buffers = 2 if angle_count * length <= STATIC_ROWS else 1

    sends = pl.pallas_call(
        functools.partial(pack_kernel, window),
        out_shape=jax.ShapeDtypeStruct(
            (slab_count, own_angles, 2 * window, local_cols), jnp.float32
        ),
        in_specs=[hbm] * 2,
        out_specs=vmem,
        scratch_shapes=[
            pltpu.VMEM((own_angles, row_total, local_cols), jnp.float32),
            pltpu.VMEM((own_angles, row_total, local_cols), jnp.float32),
            pltpu.SemaphoreType.DMA((2,)),
        ],
        compiler_params=params,
        name="pack",
    )(held(measured.transpose(0, 2, 1)), held(row_norm.transpose(0, 2, 1)))
    columns = sends[:, None]
    for bit in bits("gz")[:0:-1]:
        columns = exchange_slabs(columns, bit)

    partial = pl.pallas_call(
        functools.partial(forward_kernel, rows),
        out_shape=jax.ShapeDtypeStruct((angle_count * rows, tile_size), jnp.float32),
        in_specs=[hbm] * 5,
        out_specs=vmem,
        scratch_shapes=[
            pltpu.SMEM((angle_count,), jnp.int32),
            pltpu.SMEM((angle_count, slot_count), jnp.int32),
            pltpu.SMEM((angle_count, length), jnp.int32),
            pltpu.VMEM((lines, half_width), jnp.float32),
            pltpu.VMEM(tile_table.shape, jnp.bfloat16),
            pltpu.VMEM((lines * runs, tile_size), jnp.float32),
            pltpu.VMEM((buffers * length, tile_size), jnp.float32),
            pltpu.SemaphoreType.DMA((5,)),
        ],
        compiler_params=params,
        name="forward",
    )(held(live), held(tid), held(bid), vol, held(tile_table))

    assert lax.axis_size("row") == 2
    upper = lax.axis_index("row") == 1
    total = partial + swap(partial, "row", 1)
    blocks = total.reshape(angle_count, rows, tile_size)
    outer = jnp.where(upper, blocks[:, rows - rim :], blocks[:, :rim])
    middle = blocks[:, rim : rows - rim]
    columns = columns[None]
    for bit in bits("gx"):
        came = swap_many([outer, middle, columns], "gx", bit)
        outer, middle = outer + came[0], middle + came[1]
        columns = ordered((lax.axis_index("gx") & bit) != 0, columns, came[2], 0)
    last = slab_count - 1
    hops = [((z + 1) * 2, z * 2) for z in range(last)]
    hops += [(z * 2 + 1, z * 2 + 3) for z in range(last)]
    rims = lax.ppermute(outer.reshape(angle_count * rim, tile_size), ("gz", "row"), hops)
    outer = outer.reshape(rims.shape)

    columns = exchange_slabs(columns.transpose(1, 2, 0, 3, 4, 5), 1)[0].transpose(1, 0, 2, 3, 4)
    other_outer, other_rims, other_columns = swap_many([outer, rims, columns], "row", 1)
    own_rim = outer + other_rims
    far_rim = other_outer + rims
    head = jnp.where(upper, far_rim, own_rim)
    tail = jnp.where(upper, own_rim, far_rim)
    columns = ordered(upper, columns[:, None], other_columns[:, None], 1)
    columns = columns.reshape(-1, angle_count, 2, window, local_cols)
    columns = columns.transpose(2, 1, 3, 0, 4).reshape(2, angle_count * rows, tile_size)

    made = pl.pallas_call(
        functools.partial(backward_kernel, rows),
        out_shape=jax.ShapeDtypeStruct((lines, half_width), jnp.float32),
        in_specs=[smem, smem] + [vmem] * 7 + [hbm] * 2,
        out_specs=hbm,
        scratch_shapes=[
            pltpu.VMEM((angle_count, rows, tile_size), jnp.bfloat16),
            pltpu.VMEM((high, angle_count * length), jnp.bfloat16),
            pltpu.VMEM((angle_count * length, tile_size), jnp.bfloat16),
            pltpu.VMEM((angle_count * length, tile_size), jnp.bfloat16),
            pltpu.VMEM((lines, half_width), jnp.float32),
            pltpu.VMEM((lines, half_width), jnp.float32),
            pltpu.VMEM((lines, half_width), jnp.float32),
            pltpu.VMEM((high, lines // high * half_width), jnp.float32),
            pltpu.SemaphoreType.DMA((2 + lines // high,)),
        ],
        compiler_params=params,
        name="backward",
    )(
        live, tid, bid, head, middle.reshape(-1, tile_size), tail, columns[0], columns[1],
        tile_table, vol, col,
    )
    return made.reshape(slab_depth, column_width, half_width)


def solution(mesh):
    placed = (
        P(("grp", "gz"), "gx", "row"),
        P(),
        P("gz", "gx", "row", None, None),
        P("gz", "gx", "row", None, None),
        P("gz", "gx", "row", None),
        P(("grp", "gz"), ("gx", "row"), None),
        P("gz", ("gx", "row"), None),
        P("gz", "gx", "row"),
    )

    return jax.shard_map(
        on_device,
        mesh=mesh,
        in_specs=placed,
        out_specs=P(("grp", "gz"), "gx", "row"),
        check_vma=False,
    )
```

```python
import functools
import math

import jax
import jax.numpy as jnp
from jax import lax
from jax.experimental import pallas as pl
from jax.experimental.pallas import tpu as pltpu
from jax.sharding import PartitionSpec as P

ONE_HOT = 256
GROUP = 8
STATIC_ROWS = 4096
VMEM_LIMIT = 16 * 1024 * 1024


def pack_kernel(window, target_in, weight_in, sends, target, weight, sems):
    copies = [
        pltpu.make_async_copy(target_in, target, sems.at[0]),
        pltpu.make_async_copy(weight_in, weight, sems.at[1]),
    ]
    for copy in copies:
        copy.start()
    sends[...] = jnp.zeros_like(sends)
    for copy in copies:
        copy.wait()
    slabs = sends.shape[0]
    depth = window - 2
    for s in range(slabs):
        low, high = max(s * depth - 1, 0), min(s * depth + depth + 1, slabs * depth)
        skip = low - (s * depth - 1)
        for own in range(target.shape[0]):
            for at, data in ((0, target), (window, weight)):
                sends[s, own, at + skip : at + skip + high - low, :] = data[own, low:high, :]


def forward_kernel(
    rows, live_in, tid_in, bid_in, vol_in, tiles_in, out,
    live, tid, bid, vol, tiles, vox, picked, sems,
):
    angles, slots = tid.shape
    tile = tiles.shape[1]
    lines, width = vol.shape
    runs = width // tile
    pairs = ((bid_in, bid), (live_in, live), (tid_in, tid), (vol_in, vol), (tiles_in, tiles))
    copies = [pltpu.make_async_copy(a, b, sems.at[i]) for i, (a, b) in enumerate(pairs)]
    for copy in copies:
        copy.start()
    copies[3].wait()
    step = 8
    for run in range(runs):
        for line in range(0, lines, step):
            vox[pl.ds(line * runs + run, step, stride=runs), :] = vol[
                line : line + step, run * tile : (run + 1) * tile
            ]
    for copy in copies[:3]:
        copy.wait()

    def gather(a, at):
        for j in range(slots * rows):
            picked[at + j : at + j + 1, :] = vox[pl.ds(bid[a, j], 1), :]

    def project(a, at):
        count = live[a]
        total = jnp.zeros((rows, tile), jnp.float32)
        for g in range(0, slots, GROUP):
            left, right = [], []
            for k in range(g, g + GROUP):
                part = picked[at + k * rows : at + (k + 1) * rows, :]
                left.append(jnp.where(k < count, part, 0.0).astype(jnp.bfloat16))
                right.append(tiles[tid[a, k]])
            total += lax.dot_general(
                jnp.concatenate(left, axis=1),
                jnp.concatenate(right, axis=1),
                (((1,), (1,)), ((), ())),
                preferred_element_type=jnp.float32,
            )
        return total

    length = slots * rows
    if angles * length <= STATIC_ROWS:
        gather(0, 0)
        copies[4].wait()
        for a in range(angles):

            @pl.when(live[a] >= 0)
            def _():
                if a + 1 < angles:
                    gather(a + 1, (a + 1) % 2 * length)
                out[a * rows : (a + 1) * rows, :] = project(a, a % 2 * length)

    else:
        copies[4].wait()

        def project_angle(a, carry):
            gather(a, 0)
            out[pl.ds(pl.multiple_of(a * rows, 8), rows), :] = project(a, 0)
            return carry

        lax.fori_loop(0, angles, project_angle, 0)


def backward_kernel(
    rows, joined, live, tid, bid, head, middle, tail, columns, tiles, vol_in, col_in, out_in,
    target, weight, res, hot, code, spread, vol, col, out, total, sems,
):
    angles, slots = tid.shape
    tile = tiles.shape[1]
    lines, width = vol.shape
    runs = width // tile
    high = hot.shape[0]
    length = slots * rows
    reads = [
        pltpu.make_async_copy(vol_in, vol, sems.at[0]),
        pltpu.make_async_copy(col_in, col, sems.at[1]),
    ]
    for copy in reads:
        copy.start()
    if joined:
        count = columns.shape[0]
        window = rows // count
        for q in range(count):
            for a in range(angles):
                there = pl.ds(a * rows + q, window, stride=count)
                at = a * 2 * window
                target[there, :] = columns[q, at : at + window, :]
                weight[there, :] = columns[q, at + window : at + 2 * window, :]
    else:
        target[...] = columns[0]
        weight[...] = columns[1]
    for a in range(angles):
        parts = []
        for part in (head, middle, tail):
            size = part.shape[0] // angles
            parts.append(part[a * size : (a + 1) * size, :])
        here = slice(a * rows, (a + 1) * rows)
        error = target[here, :] - jnp.concatenate(parts, axis=0)
        res[a] = (weight[here, :] * error).astype(jnp.bfloat16)

    place = lax.broadcasted_iota(jnp.int32, (high, tile), 0).astype(jnp.bfloat16)
    position = lax.broadcasted_iota(jnp.int32, (1, tile), 1)
    for a in range(angles):
        groups = []
        for c in range(0, length, tile):
            block = bid[a : a + 1, c : c + tile]
            line = block // runs
            low = (line % high).astype(jnp.bfloat16)
            hot[:, a * length + c : a * length + c + tile] = jnp.where(
                place == low, jnp.bfloat16(1), jnp.bfloat16(0)
            )
            group = (line // high) * runs + block % runs
            groups.append(jnp.where(position + c < live[a] * rows, group, -1))
        pad = -len(groups) % 8
        groups += [jnp.zeros((1, tile), jnp.int32)] * pad
        turned = jnp.concatenate(groups, axis=0).astype(jnp.float32).T
        for i in range(length // tile):
            wide = jnp.broadcast_to(turned[:, i : i + 1], (tile, tile))
            code[a * length + i * tile : a * length + (i + 1) * tile, :] = wide.astype(
                jnp.bfloat16
            )

    def spread_pair(values, a, k, at):
        pair = jnp.concatenate([tiles[tid[a, k]], tiles[tid[a, k + 1]]], axis=1)
        made = jnp.dot(values, pair, preferred_element_type=jnp.float32)
        both = jnp.concatenate([made[:, :tile], made[:, tile:]], axis=0)
        spread[pl.ds(at, 2 * rows), :] = both.astype(jnp.bfloat16)

    def add_part(at, size, first, count):
        values = spread[pl.ds(at, size), :]
        groups = code[pl.ds(at, size), :]
        right = jnp.concatenate(
            [
                jnp.where(groups == jnp.bfloat16(g), values, jnp.bfloat16(0))
                for g in range(first * runs, (first + count) * runs)
            ],
            axis=1,
        )
        return jnp.dot(hot[:, pl.ds(at, size)], right, preferred_element_type=jnp.float32)

    chunks = lines // high
    writes = []

    def finish(first, count, made):
        for i in range(count):
            here = pl.ds((first + i) * high, high)
            out[here, :] = vol[here, :] + col[here, :] * made[:, i * width : (i + 1) * width]
            copy = pltpu.make_async_copy(
                out.at[here, :], out_in.at[here, :], sems.at[2 + first + i]
            )
            copy.start()
            writes.append(copy)

    if angles * length <= STATIC_ROWS:
        for a in range(angles):
            values = res[a]
            for k in range(0, slots, 2):
                spread_pair(values, a, k, (a * slots + k) * rows)
        made = add_part(0, angles * length, 0, chunks)
        for copy in reads:
            copy.wait()
        finish(0, chunks, made)
    else:

        def step(a, carry):
            values = res[a]
            base = pl.multiple_of(a * length, 256)
            for k in range(0, slots, 2):
                spread_pair(values, a, k, base + k * rows)
            total[...] += add_part(base, length, 0, chunks)
            return carry

        total[...] = jnp.zeros_like(total)
        lax.fori_loop(0, angles, step, 0)
        for copy in reads:
            copy.wait()
        finish(0, chunks, total[...])
    for copy in writes:
        copy.wait()


def swap(values, axis, bit):
    return lax.ppermute(values, axis, [(i, i ^ bit) for i in range(lax.axis_size(axis))])


def move_many(arrays, axis, hops):
    if len({array.shape[-1] for array in arrays}) > 1:
        return [lax.ppermute(array, axis, hops) for array in arrays]
    width = arrays[0].shape[-1]
    joined = jnp.concatenate([a.reshape(-1, width) for a in arrays], axis=0)
    came = lax.ppermute(joined, axis, hops)
    out, at = [], 0
    for array in arrays:
        count = array.size // width
        out.append(came[at : at + count].reshape(array.shape))
        at += count
    return out


def swap_many(arrays, axis, bit):
    return move_many(arrays, axis, [(i, i ^ bit) for i in range(lax.axis_size(axis))])


def bits(axis):
    return [1 << i for i in range((lax.axis_size(axis) - 1).bit_length())]


def ordered(mine_high, own, other, axis):
    return jnp.concatenate(
        [jnp.where(mine_high, other, own), jnp.where(mine_high, own, other)], axis=axis
    )


def exchange_slabs(parts, bit):
    high = (lax.axis_index("gz") & bit) != 0
    count = parts.shape[0] // 2
    halves = parts.reshape((2, count) + parts.shape[1:])
    keep = jnp.where(high, halves[1], halves[0])
    give = jnp.where(high, halves[0], halves[1])
    with jax.named_scope(f"slab{bit}"):
        came = swap(give, "gz", bit)
    low, up = jnp.where(high, came, keep), jnp.where(high, keep, came)
    both = jnp.stack([low, up], axis=2)
    return both.reshape((count, parts.shape[1] * 2) + parts.shape[2:])


def on_device(volume, tile_table, tile_ids, block_ids, live_slots, measured, row_norm, col_norm):
    slab_depth, column_width, half_width = volume.shape
    tile_size = tile_table.shape[1]
    angle_count, slot_count = tile_ids.shape[3:]
    window = slab_depth + 2
    block_cols = block_ids.shape[4] // (slot_count * window)
    rows = window * block_cols
    rim = 2 * block_cols
    length = slot_count * rows
    lines = slab_depth * column_width
    runs = half_width // tile_size
    high = math.gcd(lines, ONE_HOT)
    slab_count = lax.axis_size("gz")
    own_angles, local_cols, row_total = measured.shape

    def held(array):
        return pltpu.with_memory_space_constraint(array, pltpu.HBM)

    tid = tile_ids.reshape(angle_count, slot_count)
    bid = block_ids.reshape(angle_count, length)
    live = live_slots.reshape(angle_count)
    vol = held(volume.reshape(lines, half_width))
    col = held(col_norm.reshape(lines, half_width))

    smem = pl.BlockSpec(memory_space=pltpu.SMEM)
    vmem = pl.BlockSpec(memory_space=pltpu.VMEM)
    hbm = pl.BlockSpec(memory_space=pltpu.HBM)
    params = pltpu.CompilerParams(vmem_limit_bytes=VMEM_LIMIT)
    buffers = 2 if angle_count * length <= STATIC_ROWS else 1

    sends = pl.pallas_call(
        functools.partial(pack_kernel, window),
        out_shape=jax.ShapeDtypeStruct(
            (slab_count, own_angles, 2 * window, local_cols), jnp.float32
        ),
        in_specs=[hbm] * 2,
        out_specs=vmem,
        scratch_shapes=[
            pltpu.VMEM((own_angles, row_total, local_cols), jnp.float32),
            pltpu.VMEM((own_angles, row_total, local_cols), jnp.float32),
            pltpu.SemaphoreType.DMA((2,)),
        ],
        compiler_params=params,
        name="pack",
    )(held(measured.transpose(0, 2, 1)), held(row_norm.transpose(0, 2, 1)))
    columns = sends[:, None]
    for bit in bits("gz")[:0:-1]:
        columns = exchange_slabs(columns, bit)

    partial = pl.pallas_call(
        functools.partial(forward_kernel, rows),
        out_shape=jax.ShapeDtypeStruct((angle_count * rows, tile_size), jnp.float32),
        in_specs=[hbm] * 5,
        out_specs=vmem,
        scratch_shapes=[
            pltpu.SMEM((angle_count,), jnp.int32),
            pltpu.SMEM((angle_count, slot_count), jnp.int32),
            pltpu.SMEM((angle_count, length), jnp.int32),
            pltpu.VMEM((lines, half_width), jnp.float32),
            pltpu.VMEM(tile_table.shape, jnp.bfloat16),
            pltpu.VMEM((lines * runs, tile_size), jnp.float32),
            pltpu.VMEM((buffers * length, tile_size), jnp.float32),
            pltpu.SemaphoreType.DMA((5,)),
        ],
        compiler_params=params,
        name="forward",
    )(held(live), held(tid), held(bid), vol, held(tile_table))

    assert lax.axis_size("row") == 2
    upper = lax.axis_index("row") == 1
    odd = (lax.axis_index("gz") & 1) == 1
    faces = upper != odd
    keep = jnp.where(odd, columns[1], columns[0])
    give = jnp.where(odd, columns[0], columns[1])
    columns = jnp.where(faces, give, keep)
    with jax.named_scope("rowsum"):
        came = swap_many([partial, jnp.where(faces, keep, give)], "row", 1)
    total = partial + came[0]
    columns = ordered(upper, columns[None], came[1][None], 0)[None]
    blocks = total.reshape(angle_count, rows, tile_size)
    outer = jnp.where(upper, blocks[:, rows - rim :], blocks[:, :rim])
    middle = blocks[:, rim : rows - rim]
    for bit in bits("gx"):
        with jax.named_scope(f"gxsum{bit}"):
            came = swap_many([outer, middle, columns], "gx", bit)
        outer, middle = outer + came[0], middle + came[1]
        columns = ordered((lax.axis_index("gx") & bit) != 0, columns, came[2], 0)
    last = slab_count - 1
    hops = [((z + 1) * 2, z * 2) for z in range(last)]
    hops += [(z * 2 + 1, z * 2 + 3) for z in range(last)]
    with jax.named_scope("rims"):
        rims, came = move_many([outer, columns], ("gz", "row"), hops)
    columns = jnp.stack([jnp.where(odd, came, columns), jnp.where(odd, columns, came)], axis=3)
    with jax.named_scope("finish"):
        came = swap_many([outer, rims, columns], "row", 1)
    own_rim = outer + came[1]
    far_rim = came[0] + rims
    head = jnp.where(upper, far_rim, own_rim).reshape(-1, tile_size)
    tail = jnp.where(upper, own_rim, far_rim).reshape(-1, tile_size)
    columns = jnp.where(faces, came[2], columns)
    joined = local_cols == tile_size
    if joined:
        columns = columns.reshape(block_cols, angle_count * 2 * window, tile_size)
    else:
        columns = columns.reshape(-1, angle_count, 2, window, local_cols)
        columns = columns.transpose(2, 1, 3, 0, 4).reshape(2, angle_count * rows, tile_size)

    made = pl.pallas_call(
        functools.partial(backward_kernel, rows, joined),
        out_shape=jax.ShapeDtypeStruct((lines, half_width), jnp.float32),
        in_specs=[smem, smem] + [vmem] * 6 + [hbm] * 2,
        out_specs=hbm,
        scratch_shapes=[
            pltpu.VMEM((angle_count * rows, tile_size), jnp.float32),
            pltpu.VMEM((angle_count * rows, tile_size), jnp.float32),
            pltpu.VMEM((angle_count, rows, tile_size), jnp.bfloat16),
            pltpu.VMEM((high, angle_count * length), jnp.bfloat16),
            pltpu.VMEM((angle_count * length, tile_size), jnp.bfloat16),
            pltpu.VMEM((angle_count * length, tile_size), jnp.bfloat16),
            pltpu.VMEM((lines, half_width), jnp.float32),
            pltpu.VMEM((lines, half_width), jnp.float32),
            pltpu.VMEM((lines, half_width), jnp.float32),
            pltpu.VMEM((high, lines // high * half_width), jnp.float32),
            pltpu.SemaphoreType.DMA((2 + lines // high,)),
        ],
        compiler_params=params,
        name="backward",
    )(
        live, tid, bid, head, middle.reshape(-1, tile_size), tail, columns, tile_table, vol, col,
    )
    return made.reshape(slab_depth, column_width, half_width)


def solution(mesh):
    placed = (
        P(("grp", "gz"), "gx", "row"),
        P(),
        P("gz", "gx", "row", None, None),
        P("gz", "gx", "row", None, None),
        P("gz", "gx", "row", None),
        P(("grp", "gz"), ("gx", "row"), None),
        P("gz", ("gx", "row"), None),
        P("gz", "gx", "row"),
    )

    return jax.shard_map(
        on_device,
        mesh=mesh,
        in_specs=placed,
        out_specs=P(("grp", "gz"), "gx", "row"),
        check_vma=False,
    )
```

```python
import functools
import math

import jax
import jax.numpy as jnp
from jax import lax
from jax.experimental import pallas as pl
from jax.experimental.pallas import tpu as pltpu
from jax.sharding import PartitionSpec as P

ONE_HOT = 256
GROUP = 8
STATIC_ROWS = 4096
VMEM_LIMIT = 16 * 1024 * 1024


def pack_kernel(window, target_in, weight_in, sends, target, weight, sems):
    copies = [
        pltpu.make_async_copy(target_in, target, sems.at[0]),
        pltpu.make_async_copy(weight_in, weight, sems.at[1]),
    ]
    for copy in copies:
        copy.start()
    sends[...] = jnp.zeros_like(sends)
    for copy in copies:
        copy.wait()
    slabs = sends.shape[0]
    depth = window - 2
    for s in range(slabs):
        low, high = max(s * depth - 1, 0), min(s * depth + depth + 1, slabs * depth)
        skip = low - (s * depth - 1)
        for own in range(target.shape[0]):
            for at, data in ((0, target), (window, weight)):
                sends[s, own, at + skip : at + skip + high - low, :] = data[own, low:high, :]


def forward_kernel(
    rows, live_in, tid_in, bid_in, vol_in, tiles_in, out,
    live, tid, bid, vol, tiles, vox, picked, sems,
):
    angles, slots = tid.shape
    tile = tiles.shape[1]
    lines, width = vol.shape
    runs = width // tile
    pairs = ((bid_in, bid), (live_in, live), (tid_in, tid), (vol_in, vol), (tiles_in, tiles))
    copies = [pltpu.make_async_copy(a, b, sems.at[i]) for i, (a, b) in enumerate(pairs)]
    for copy in copies:
        copy.start()
    copies[3].wait()
    step = 8
    for run in range(runs):
        for line in range(0, lines, step):
            vox[pl.ds(line * runs + run, step, stride=runs), :] = vol[
                line : line + step, run * tile : (run + 1) * tile
            ]
    for copy in copies[:3]:
        copy.wait()

    def gather(a, at):
        for j in range(slots * rows):
            picked[at + j : at + j + 1, :] = vox[pl.ds(bid[a, j], 1), :]

    def project(a, at):
        count = live[a]
        total = jnp.zeros((rows, tile), jnp.float32)
        for g in range(0, slots, GROUP):
            left, right = [], []
            for k in range(g, g + GROUP):
                part = picked[at + k * rows : at + (k + 1) * rows, :]
                left.append(jnp.where(k < count, part, 0.0).astype(jnp.bfloat16))
                right.append(tiles[tid[a, k]])
            total += lax.dot_general(
                jnp.concatenate(left, axis=1),
                jnp.concatenate(right, axis=1),
                (((1,), (1,)), ((), ())),
                preferred_element_type=jnp.float32,
            )
        return total

    length = slots * rows
    if angles * length <= STATIC_ROWS:
        gather(0, 0)
        copies[4].wait()
        for a in range(angles):

            @pl.when(live[a] >= 0)
            def _():
                if a + 1 < angles:
                    gather(a + 1, (a + 1) % 2 * length)
                out[a * rows : (a + 1) * rows, :] = project(a, a % 2 * length)

    else:
        copies[4].wait()

        def project_angle(a, carry):
            gather(a, 0)
            out[pl.ds(pl.multiple_of(a * rows, 8), rows), :] = project(a, 0)
            return carry

        lax.fori_loop(0, angles, project_angle, 0)


def backward_kernel(
    rows, joined, live, tid, bid, head, middle, tail, columns, tiles, vol_in, col_in, out_in,
    target, weight, res, hot, code, spread, vol, col, out, total, sems,
):
    angles, slots = tid.shape
    tile = tiles.shape[1]
    lines, width = vol.shape
    runs = width // tile
    high = hot.shape[0]
    length = slots * rows
    reads = [
        pltpu.make_async_copy(vol_in, vol, sems.at[0]),
        pltpu.make_async_copy(col_in, col, sems.at[1]),
    ]
    for copy in reads:
        copy.start()
    if joined:
        count = columns.shape[0]
        window = rows // count
        for q in range(count):
            for a in range(angles):
                there = pl.ds(a * rows + q, window, stride=count)
                at = a * 2 * window
                target[there, :] = columns[q, at : at + window, :]
                weight[there, :] = columns[q, at + window : at + 2 * window, :]
    else:
        target[...] = columns[0]
        weight[...] = columns[1]
    for a in range(angles):
        parts = []
        for part in (head, middle, tail):
            size = part.shape[0] // angles
            parts.append(part[a * size : (a + 1) * size, :])
        here = slice(a * rows, (a + 1) * rows)
        error = target[here, :] - jnp.concatenate(parts, axis=0)
        res[a] = (weight[here, :] * error).astype(jnp.bfloat16)

    place = lax.broadcasted_iota(jnp.int32, (high, tile), 0).astype(jnp.bfloat16)
    position = lax.broadcasted_iota(jnp.int32, (1, tile), 1)
    static = angles * length <= STATIC_ROWS
    codes = []
    for a in range(angles):
        groups = []
        for c in range(0, length, tile):
            block = bid[a : a + 1, c : c + tile]
            line = block // runs
            low = (line % high).astype(jnp.bfloat16)
            hot[:, a * length + c : a * length + c + tile] = jnp.where(
                place == low, jnp.bfloat16(1), jnp.bfloat16(0)
            )
            group = (line // high) * runs + block % runs
            groups.append(jnp.where(position + c < live[a] * rows, group, -1))
        pad = -len(groups) % 8
        groups += [jnp.zeros((1, tile), jnp.int32)] * pad
        turned = jnp.concatenate(groups, axis=0).astype(jnp.float32).T
        for i in range(length // tile):
            wide = jnp.broadcast_to(turned[:, i : i + 1], (tile, tile))
            if static:
                codes.append(wide.astype(jnp.bfloat16))
            else:
                here = slice(a * length + i * tile, a * length + (i + 1) * tile)
                code[here, :] = wide.astype(jnp.bfloat16)

    def spread_pair(values, a, k):
        pair = jnp.concatenate([tiles[tid[a, k]], tiles[tid[a, k + 1]]], axis=1)
        made = jnp.dot(values, pair, preferred_element_type=jnp.float32)
        both = jnp.concatenate([made[:, :tile], made[:, tile:]], axis=0)
        return both.astype(jnp.bfloat16)

    def add_part(values, groups, chosen):
        right = jnp.concatenate(
            [
                jnp.where(groups == jnp.bfloat16(g), values, jnp.bfloat16(0))
                for g in range(chunks * runs)
            ],
            axis=1,
        )
        return jnp.dot(chosen, right, preferred_element_type=jnp.float32)

    chunks = lines // high
    writes = []

    def finish(first, count, made):
        for i in range(count):
            here = pl.ds((first + i) * high, high)
            out[here, :] = vol[here, :] + col[here, :] * made[:, i * width : (i + 1) * width]
            copy = pltpu.make_async_copy(
                out.at[here, :], out_in.at[here, :], sems.at[2 + first + i]
            )
            copy.start()
            writes.append(copy)

    if static:
        values = []
        for a in range(angles):
            for k in range(0, slots, 2):
                values.append(spread_pair(res[a], a, k))
        made = add_part(
            jnp.concatenate(values, axis=0), jnp.concatenate(codes, axis=0), hot[...]
        )
        for copy in reads:
            copy.wait()
        finish(0, chunks, made)
    else:

        def step(a, carry):
            values = res[a]
            base = pl.multiple_of(a * length, 256)
            for k in range(0, slots, 2):
                spread[k * rows : (k + 2) * rows, :] = spread_pair(values, a, k)
            total[...] += add_part(
                spread[...], code[pl.ds(base, length), :], hot[:, pl.ds(base, length)]
            )
            return carry

        total[...] = jnp.zeros_like(total)
        lax.fori_loop(0, angles, step, 0)
        for copy in reads:
            copy.wait()
        finish(0, chunks, total[...])
    for copy in writes:
        copy.wait()


def swap(values, axis, bit):
    return lax.ppermute(values, axis, [(i, i ^ bit) for i in range(lax.axis_size(axis))])


def move_many(arrays, axis, hops):
    if len({array.shape[-1] for array in arrays}) > 1:
        return [lax.ppermute(array, axis, hops) for array in arrays]
    width = arrays[0].shape[-1]
    joined = jnp.concatenate([a.reshape(-1, width) for a in arrays], axis=0)
    came = lax.ppermute(joined, axis, hops)
    out, at = [], 0
    for array in arrays:
        count = array.size // width
        out.append(came[at : at + count].reshape(array.shape))
        at += count
    return out


def swap_many(arrays, axis, bit):
    return move_many(arrays, axis, [(i, i ^ bit) for i in range(lax.axis_size(axis))])


def bits(axis):
    return [1 << i for i in range((lax.axis_size(axis) - 1).bit_length())]


def ordered(mine_high, own, other, axis):
    return jnp.concatenate(
        [jnp.where(mine_high, other, own), jnp.where(mine_high, own, other)], axis=axis
    )


def exchange_slabs(parts, bit):
    high = (lax.axis_index("gz") & bit) != 0
    count = parts.shape[0] // 2
    halves = parts.reshape((2, count) + parts.shape[1:])
    keep = jnp.where(high, halves[1], halves[0])
    give = jnp.where(high, halves[0], halves[1])
    with jax.named_scope(f"slab{bit}"):
        came = swap(give, "gz", bit)
    low, up = jnp.where(high, came, keep), jnp.where(high, keep, came)
    both = jnp.stack([low, up], axis=2)
    return both.reshape((count, parts.shape[1] * 2) + parts.shape[2:])


def on_device(volume, tile_table, tile_ids, block_ids, live_slots, measured, row_norm, col_norm):
    slab_depth, column_width, half_width = volume.shape
    tile_size = tile_table.shape[1]
    angle_count, slot_count = tile_ids.shape[3:]
    window = slab_depth + 2
    block_cols = block_ids.shape[4] // (slot_count * window)
    rows = window * block_cols
    rim = 2 * block_cols
    length = slot_count * rows
    lines = slab_depth * column_width
    runs = half_width // tile_size
    high = math.gcd(lines, ONE_HOT)
    slab_count = lax.axis_size("gz")
    own_angles, local_cols, row_total = measured.shape

    def held(array):
        return pltpu.with_memory_space_constraint(array, pltpu.HBM)

    tid = tile_ids.reshape(angle_count, slot_count)
    bid = block_ids.reshape(angle_count, length)
    live = live_slots.reshape(angle_count)
    vol = held(volume.reshape(lines, half_width))
    col = held(col_norm.reshape(lines, half_width))

    smem = pl.BlockSpec(memory_space=pltpu.SMEM)
    vmem = pl.BlockSpec(memory_space=pltpu.VMEM)
    hbm = pl.BlockSpec(memory_space=pltpu.HBM)
    params = pltpu.CompilerParams(vmem_limit_bytes=VMEM_LIMIT)
    buffers = 2 if angle_count * length <= STATIC_ROWS else 1

    sends = pl.pallas_call(
        functools.partial(pack_kernel, window),
        out_shape=jax.ShapeDtypeStruct(
            (slab_count, own_angles, 2 * window, local_cols), jnp.float32
        ),
        in_specs=[hbm] * 2,
        out_specs=vmem,
        scratch_shapes=[
            pltpu.VMEM((own_angles, row_total, local_cols), jnp.float32),
            pltpu.VMEM((own_angles, row_total, local_cols), jnp.float32),
            pltpu.SemaphoreType.DMA((2,)),
        ],
        compiler_params=params,
        name="pack",
    )(held(measured.transpose(0, 2, 1)), held(row_norm.transpose(0, 2, 1)))
    columns = sends[:, None]
    for bit in bits("gz")[:0:-1]:
        columns = exchange_slabs(columns, bit)

    partial = pl.pallas_call(
        functools.partial(forward_kernel, rows),
        out_shape=jax.ShapeDtypeStruct((angle_count * rows, tile_size), jnp.float32),
        in_specs=[hbm] * 5,
        out_specs=vmem,
        scratch_shapes=[
            pltpu.SMEM((angle_count,), jnp.int32),
            pltpu.SMEM((angle_count, slot_count), jnp.int32),
            pltpu.SMEM((angle_count, length), jnp.int32),
            pltpu.VMEM((lines, half_width), jnp.float32),
            pltpu.VMEM(tile_table.shape, jnp.bfloat16),
            pltpu.VMEM((lines * runs, tile_size), jnp.float32),
            pltpu.VMEM((buffers * length, tile_size), jnp.float32),
            pltpu.SemaphoreType.DMA((5,)),
        ],
        compiler_params=params,
        name="forward",
    )(held(live), held(tid), held(bid), vol, held(tile_table))

    assert lax.axis_size("row") == 2
    upper = lax.axis_index("row") == 1
    odd = (lax.axis_index("gz") & 1) == 1
    top = upper != odd
    keep = jnp.where(odd, columns[1], columns[0])
    give = jnp.where(odd, columns[0], columns[1])
    columns = jnp.where(upper, give, keep)
    with jax.named_scope("rowsum"):
        came = swap_many([partial, jnp.where(upper, keep, give)], "row", 1)
    total = partial + came[0]
    columns = ordered(upper, columns[None], came[1][None], 0)[None]
    blocks = total.reshape(angle_count, rows, tile_size)
    outer = jnp.where(top, blocks[:, rows - rim :], blocks[:, :rim])
    middle = blocks[:, rim : rows - rim]
    for bit in bits("gx"):
        with jax.named_scope(f"gxsum{bit}"):
            came = swap_many([outer, middle, columns], "gx", bit)
        outer, middle = outer + came[0], middle + came[1]
        columns = ordered((lax.axis_index("gx") & bit) != 0, columns, came[2], 0)
    hops = [(z * 2 + 1, (z ^ 1) * 2 + 1) for z in range(slab_count)]
    hops += [(z * 2, ((z + 1 ^ 1) - 1) * 2) for z in range(1, slab_count - 1)]
    with jax.named_scope("rims"):
        came = move_many([outer, columns], ("gz", "row"), hops)
    outer = outer + came[0]
    columns = jnp.where(upper, came[1], columns)
    with jax.named_scope("finish"):
        came = swap_many([outer, columns], "row", 1)
    head = jnp.where(top, came[0], outer).reshape(-1, tile_size)
    tail = jnp.where(top, outer, came[0]).reshape(-1, tile_size)
    low, up = jnp.where(top, came[1], columns), jnp.where(top, columns, came[1])
    columns = jnp.stack([low, up], axis=3)
    joined = local_cols == tile_size
    if joined:
        columns = columns.reshape(block_cols, angle_count * 2 * window, tile_size)
    else:
        columns = columns.reshape(-1, angle_count, 2, window, local_cols)
        columns = columns.transpose(2, 1, 3, 0, 4).reshape(2, angle_count * rows, tile_size)

    made = pl.pallas_call(
        functools.partial(backward_kernel, rows, joined),
        out_shape=jax.ShapeDtypeStruct((lines, half_width), jnp.float32),
        in_specs=[smem, smem] + [vmem] * 6 + [hbm] * 2,
        out_specs=hbm,
        scratch_shapes=[
            pltpu.VMEM((angle_count * rows, tile_size), jnp.float32),
            pltpu.VMEM((angle_count * rows, tile_size), jnp.float32),
            pltpu.VMEM((angle_count, rows, tile_size), jnp.bfloat16),
            pltpu.VMEM((high, angle_count * length), jnp.bfloat16),
            pltpu.VMEM((angle_count * length, tile_size), jnp.bfloat16),
            pltpu.VMEM((length, tile_size), jnp.bfloat16),
            pltpu.VMEM((lines, half_width), jnp.float32),
            pltpu.VMEM((lines, half_width), jnp.float32),
            pltpu.VMEM((lines, half_width), jnp.float32),
            pltpu.VMEM((high, lines // high * half_width), jnp.float32),
            pltpu.SemaphoreType.DMA((2 + lines // high,)),
        ],
        compiler_params=params,
        name="backward",
    )(
        live, tid, bid, head, middle.reshape(-1, tile_size), tail, columns, tile_table, vol, col,
    )
    return made.reshape(slab_depth, column_width, half_width)


def solution(mesh):
    placed = (
        P(("grp", "gz"), "gx", "row"),
        P(),
        P("gz", "gx", "row", None, None),
        P("gz", "gx", "row", None, None),
        P("gz", "gx", "row", None),
        P(("grp", "gz"), ("gx", "row"), None),
        P("gz", ("gx", "row"), None),
        P("gz", "gx", "row"),
    )

    return jax.shard_map(
        on_device,
        mesh=mesh,
        in_specs=placed,
        out_specs=P(("grp", "gz"), "gx", "row"),
        check_vma=False,
    )
```

```python
import functools
import math

import jax
import jax.numpy as jnp
from jax import lax
from jax.experimental import pallas as pl
from jax.experimental.pallas import tpu as pltpu
from jax.sharding import PartitionSpec as P

ONE_HOT = 256
GROUP = 8
STATIC_ROWS = 4096
VMEM_LIMIT = 16 * 1024 * 1024


def pack_kernel(window, target_in, weight_in, sends, target, weight, made, sems):
    copies = [
        pltpu.make_async_copy(target_in, target, sems.at[0]),
        pltpu.make_async_copy(weight_in, weight, sems.at[1]),
    ]
    for copy in copies:
        copy.start()
    made[...] = jnp.zeros_like(made)
    for copy in copies:
        copy.wait()
    slabs = sends.shape[0]
    depth = window - 2
    for s in range(slabs):
        low, high = max(s * depth - 1, 0), min(s * depth + depth + 1, slabs * depth)
        skip = low - (s * depth - 1)
        for own in range(target.shape[0]):
            for at, data in ((0, target), (made.shape[2] // 2, weight)):
                made[s, own, at + skip : at + skip + high - low, :] = data[own, low:high, :]
    sends[...] = made[...].astype(sends.dtype)


def forward_kernel(
    rows, live_in, tid_in, bid_in, vol_in, tiles_in, out,
    live, tid, bid, vol, tiles, vox, picked, sems,
):
    angles, slots = tid.shape
    tile = tiles.shape[1]
    lines, width = vol.shape
    runs = width // tile
    pairs = ((bid_in, bid), (live_in, live), (tid_in, tid), (vol_in, vol), (tiles_in, tiles))
    copies = [pltpu.make_async_copy(a, b, sems.at[i]) for i, (a, b) in enumerate(pairs)]
    for copy in copies:
        copy.start()
    copies[3].wait()
    step = 8
    for run in range(runs):
        for line in range(0, lines, step):
            vox[pl.ds(line * runs + run, step, stride=runs), :] = vol[
                line : line + step, run * tile : (run + 1) * tile
            ]
    for copy in copies[:3]:
        copy.wait()

    def gather(a, at):
        for j in range(slots * rows):
            picked[at + j : at + j + 1, :] = vox[pl.ds(bid[a, j], 1), :]

    def project(a, at):
        count = live[a]
        total = jnp.zeros((rows, tile), jnp.float32)
        for g in range(0, slots, GROUP):
            left, right = [], []
            for k in range(g, g + GROUP):
                part = picked[at + k * rows : at + (k + 1) * rows, :]
                left.append(jnp.where(k < count, part, 0.0).astype(jnp.bfloat16))
                right.append(tiles[tid[a, k]])
            total += lax.dot_general(
                jnp.concatenate(left, axis=1),
                jnp.concatenate(right, axis=1),
                (((1,), (1,)), ((), ())),
                preferred_element_type=jnp.float32,
            )
        return total

    length = slots * rows
    if angles * length <= STATIC_ROWS:
        gather(0, 0)
        copies[4].wait()
        for a in range(angles):

            @pl.when(live[a] >= 0)
            def _():
                if a + 1 < angles:
                    gather(a + 1, (a + 1) % 2 * length)
                out[a * rows : (a + 1) * rows, :] = project(a, a % 2 * length)

    else:
        copies[4].wait()

        def project_angle(a, carry):
            gather(a, 0)
            out[pl.ds(pl.multiple_of(a * rows, 8), rows), :] = project(a, 0)
            return carry

        lax.fori_loop(0, angles, project_angle, 0)


def backward_kernel(
    rows, joined, live, tid, bid, head, middle, tail, columns, tiles, vol_in, col_in, out_in,
    target, weight, res, hot, code, spread, vol, col, out, total, sems,
):
    angles, slots = tid.shape
    tile = tiles.shape[1]
    lines, width = vol.shape
    runs = width // tile
    high = hot.shape[0]
    length = slots * rows
    reads = [
        pltpu.make_async_copy(vol_in, vol, sems.at[0]),
        pltpu.make_async_copy(col_in, col, sems.at[1]),
    ]
    for copy in reads:
        copy.start()
    if joined:
        count = columns.shape[0]
        window = rows // count
        padded = columns.shape[1] // angles // 2
        for q in range(count):
            for a in range(angles):
                there = pl.ds(a * rows + q, window, stride=count)
                at = a * 2 * padded
                both = columns[q, at : at + 2 * padded, :].astype(jnp.float32)
                target[there, :] = both[:window]
                weight[there, :] = both[padded : padded + window]
    else:
        target[...] = columns[0].astype(jnp.float32)
        weight[...] = columns[1].astype(jnp.float32)
    for a in range(angles):
        parts = []
        for part in (head, middle, tail):
            size = part.shape[0] // angles
            parts.append(part[a * size : (a + 1) * size, :])
        here = slice(a * rows, (a + 1) * rows)
        error = target[here, :] - jnp.concatenate(parts, axis=0)
        res[a] = (weight[here, :] * error).astype(jnp.bfloat16)

    place = lax.broadcasted_iota(jnp.int32, (high, tile), 0).astype(jnp.bfloat16)
    position = lax.broadcasted_iota(jnp.int32, (1, tile), 1)
    static = angles * length <= STATIC_ROWS
    codes = []
    for a in range(angles):
        groups = []
        for c in range(0, length, tile):
            block = bid[a : a + 1, c : c + tile]
            line = block // runs
            low = (line % high).astype(jnp.bfloat16)
            hot[:, a * length + c : a * length + c + tile] = jnp.where(
                place == low, jnp.bfloat16(1), jnp.bfloat16(0)
            )
            group = (line // high) * runs + block % runs
            groups.append(jnp.where(position + c < live[a] * rows, group, -1))
        pad = -len(groups) % 8
        groups += [jnp.zeros((1, tile), jnp.int32)] * pad
        turned = jnp.concatenate(groups, axis=0).astype(jnp.float32).T
        for i in range(length // tile):
            wide = jnp.broadcast_to(turned[:, i : i + 1], (tile, tile))
            if static:
                codes.append(wide.astype(jnp.bfloat16))
            else:
                here = slice(a * length + i * tile, a * length + (i + 1) * tile)
                code[here, :] = wide.astype(jnp.bfloat16)

    def spread_pair(values, a, k):
        pair = jnp.concatenate([tiles[tid[a, k]], tiles[tid[a, k + 1]]], axis=1)
        made = jnp.dot(values, pair, preferred_element_type=jnp.float32)
        both = jnp.concatenate([made[:, :tile], made[:, tile:]], axis=0)
        return both.astype(jnp.bfloat16)

    def add_part(values, groups, chosen):
        right = jnp.concatenate(
            [
                jnp.where(groups == jnp.bfloat16(g), values, jnp.bfloat16(0))
                for g in range(chunks * runs)
            ],
            axis=1,
        )
        return jnp.dot(chosen, right, preferred_element_type=jnp.float32)

    chunks = lines // high
    writes = []

    def finish(first, count, made):
        for i in range(count):
            here = pl.ds((first + i) * high, high)
            out[here, :] = vol[here, :] + col[here, :] * made[:, i * width : (i + 1) * width]
            copy = pltpu.make_async_copy(
                out.at[here, :], out_in.at[here, :], sems.at[2 + first + i]
            )
            copy.start()
            writes.append(copy)

    if static:
        values = []
        for a in range(angles):
            for k in range(0, slots, 2):
                values.append(spread_pair(res[a], a, k))
        made = add_part(
            jnp.concatenate(values, axis=0), jnp.concatenate(codes, axis=0), hot[...]
        )
        for copy in reads:
            copy.wait()
        finish(0, chunks, made)
    else:

        def step(a, carry):
            values = res[a]
            base = pl.multiple_of(a * length, 256)
            for k in range(0, slots, 2):
                spread[k * rows : (k + 2) * rows, :] = spread_pair(values, a, k)
            total[...] += add_part(
                spread[...], code[pl.ds(base, length), :], hot[:, pl.ds(base, length)]
            )
            return carry

        total[...] = jnp.zeros_like(total)
        lax.fori_loop(0, angles, step, 0)
        for copy in reads:
            copy.wait()
        finish(0, chunks, total[...])
    for copy in writes:
        copy.wait()


def swap(values, axis, bit):
    return lax.ppermute(values, axis, [(i, i ^ bit) for i in range(lax.axis_size(axis))])


def move_many(arrays, axis, hops):
    if len({array.shape[-1] for array in arrays}) > 1:
        return [lax.ppermute(array, axis, hops) for array in arrays]
    width = arrays[0].shape[-1]
    joined = jnp.concatenate([a.reshape(-1, width) for a in arrays], axis=0)
    came = lax.ppermute(joined, axis, hops)
    out, at = [], 0
    for array in arrays:
        count = array.size // width
        out.append(came[at : at + count].reshape(array.shape))
        at += count
    return out


def swap_many(arrays, axis, bit):
    return move_many(arrays, axis, [(i, i ^ bit) for i in range(lax.axis_size(axis))])


def bits(axis):
    return [1 << i for i in range((lax.axis_size(axis) - 1).bit_length())]


def ordered(mine_high, own, other, axis):
    return jnp.concatenate(
        [jnp.where(mine_high, other, own), jnp.where(mine_high, own, other)], axis=axis
    )


def exchange_slabs(parts, bit):
    high = (lax.axis_index("gz") & bit) != 0
    count = parts.shape[0] // 2
    halves = parts.reshape((2, count) + parts.shape[1:])
    keep = jnp.where(high, halves[1], halves[0])
    give = jnp.where(high, halves[0], halves[1])
    with jax.named_scope(f"slab{bit}"):
        came = swap(give, "gz", bit)
    low, up = jnp.where(high, came, keep), jnp.where(high, keep, came)
    both = jnp.stack([low, up], axis=2)
    return both.reshape((count, parts.shape[1] * 2) + parts.shape[2:])


def on_device(volume, tile_table, tile_ids, block_ids, live_slots, measured, row_norm, col_norm):
    slab_depth, column_width, half_width = volume.shape
    tile_size = tile_table.shape[1]
    angle_count, slot_count = tile_ids.shape[3:]
    window = slab_depth + 2
    block_cols = block_ids.shape[4] // (slot_count * window)
    rows = window * block_cols
    rim = 2 * block_cols
    padded = -(-window // 8) * 8
    length = slot_count * rows
    lines = slab_depth * column_width
    runs = half_width // tile_size
    high = math.gcd(lines, ONE_HOT)
    slab_count = lax.axis_size("gz")
    own_angles, local_cols, row_total = measured.shape

    def held(array):
        return pltpu.with_memory_space_constraint(array, pltpu.HBM)

    tid = tile_ids.reshape(angle_count, slot_count)
    bid = block_ids.reshape(angle_count, length)
    live = live_slots.reshape(angle_count)
    vol = held(volume.reshape(lines, half_width))
    col = held(col_norm.reshape(lines, half_width))

    smem = pl.BlockSpec(memory_space=pltpu.SMEM)
    vmem = pl.BlockSpec(memory_space=pltpu.VMEM)
    hbm = pl.BlockSpec(memory_space=pltpu.HBM)
    params = pltpu.CompilerParams(vmem_limit_bytes=VMEM_LIMIT)
    buffers = 2 if angle_count * length <= STATIC_ROWS else 1

    sends = pl.pallas_call(
        functools.partial(pack_kernel, window),
        out_shape=jax.ShapeDtypeStruct(
            (slab_count, own_angles, 2 * padded, local_cols), jnp.bfloat16
        ),
        in_specs=[hbm] * 2,
        out_specs=vmem,
        scratch_shapes=[
            pltpu.VMEM((own_angles, row_total, local_cols), jnp.float32),
            pltpu.VMEM((own_angles, row_total, local_cols), jnp.float32),
            pltpu.VMEM((slab_count, own_angles, 2 * padded, local_cols), jnp.float32),
            pltpu.SemaphoreType.DMA((2,)),
        ],
        compiler_params=params,
        name="pack",
    )(held(measured.transpose(0, 2, 1)), held(row_norm.transpose(0, 2, 1)))
    columns = sends[:, None]
    for bit in bits("gz")[:0:-1]:
        columns = exchange_slabs(columns, bit)

    partial = pl.pallas_call(
        functools.partial(forward_kernel, rows),
        out_shape=jax.ShapeDtypeStruct((angle_count * rows, tile_size), jnp.float32),
        in_specs=[hbm] * 5,
        out_specs=vmem,
        scratch_shapes=[
            pltpu.SMEM((angle_count,), jnp.int32),
            pltpu.SMEM((angle_count, slot_count), jnp.int32),
            pltpu.SMEM((angle_count, length), jnp.int32),
            pltpu.VMEM((lines, half_width), jnp.float32),
            pltpu.VMEM(tile_table.shape, jnp.bfloat16),
            pltpu.VMEM((lines * runs, tile_size), jnp.float32),
            pltpu.VMEM((buffers * length, tile_size), jnp.float32),
            pltpu.SemaphoreType.DMA((5,)),
        ],
        compiler_params=params,
        name="forward",
    )(held(live), held(tid), held(bid), vol, held(tile_table))

    assert lax.axis_size("row") == 2
    upper = lax.axis_index("row") == 1
    odd = (lax.axis_index("gz") & 1) == 1
    top = upper != odd
    keep = jnp.where(odd, columns[1], columns[0])
    give = jnp.where(odd, columns[0], columns[1])
    columns = jnp.where(upper, give, keep)
    with jax.named_scope("rowsum"):
        passed = jnp.where(upper, keep, give).astype(jnp.float32)
        came = swap_many([partial, passed], "row", 1)
    total = partial + came[0]
    columns = ordered(upper, columns[None], came[1][None].astype(jnp.bfloat16), 0)[None]
    blocks = total.reshape(angle_count, rows, tile_size)
    outer = jnp.where(top, blocks[:, rows - rim :], blocks[:, :rim])
    middle = blocks[:, rim : rows - rim]
    for bit in bits("gx"):
        with jax.named_scope(f"gxsum{bit}"):
            parts = [outer.astype(jnp.bfloat16), middle.astype(jnp.bfloat16), columns]
            came = swap_many(parts, "gx", bit)
        outer = outer + came[0].astype(jnp.float32)
        middle = middle + came[1].astype(jnp.float32)
        columns = ordered((lax.axis_index("gx") & bit) != 0, columns, came[2], 0)
    hops = [(z * 2 + 1, (z ^ 1) * 2 + 1) for z in range(slab_count)]
    hops += [(z * 2, ((z + 1 ^ 1) - 1) * 2) for z in range(1, slab_count - 1)]
    with jax.named_scope("rims"):
        came = move_many([outer.astype(jnp.bfloat16), columns], ("gz", "row"), hops)
    outer = outer + came[0].astype(jnp.float32)
    columns = jnp.where(upper, came[1], columns)
    with jax.named_scope("finish"):
        came = swap_many([outer.astype(jnp.bfloat16), columns], "row", 1)
    far = came[0].astype(jnp.float32)
    head = jnp.where(top, far, outer).reshape(-1, tile_size)
    tail = jnp.where(top, outer, far).reshape(-1, tile_size)
    low, up = jnp.where(top, came[1], columns), jnp.where(top, columns, came[1])
    columns = jnp.stack([low, up], axis=3)
    joined = local_cols == tile_size
    if joined:
        columns = columns.reshape(block_cols, angle_count * 2 * padded, tile_size)
    else:
        columns = columns.reshape(-1, angle_count, 2, padded, local_cols)[:, :, :, :window]
        columns = columns.transpose(2, 1, 3, 0, 4).reshape(2, angle_count * rows, tile_size)

    made = pl.pallas_call(
        functools.partial(backward_kernel, rows, joined),
        out_shape=jax.ShapeDtypeStruct((lines, half_width), jnp.float32),
        in_specs=[smem, smem] + [vmem] * 6 + [hbm] * 2,
        out_specs=hbm,
        scratch_shapes=[
            pltpu.VMEM((angle_count * rows, tile_size), jnp.float32),
            pltpu.VMEM((angle_count * rows, tile_size), jnp.float32),
            pltpu.VMEM((angle_count, rows, tile_size), jnp.bfloat16),
            pltpu.VMEM((high, angle_count * length), jnp.bfloat16),
            pltpu.VMEM((angle_count * length, tile_size), jnp.bfloat16),
            pltpu.VMEM((length, tile_size), jnp.bfloat16),
            pltpu.VMEM((lines, half_width), jnp.float32),
            pltpu.VMEM((lines, half_width), jnp.float32),
            pltpu.VMEM((lines, half_width), jnp.float32),
            pltpu.VMEM((high, lines // high * half_width), jnp.float32),
            pltpu.SemaphoreType.DMA((2 + lines // high,)),
        ],
        compiler_params=params,
        name="backward",
    )(
        live, tid, bid, head, middle.reshape(-1, tile_size), tail, columns, tile_table, vol, col,
    )
    return made.reshape(slab_depth, column_width, half_width)


def solution(mesh):
    placed = (
        P(("grp", "gz"), "gx", "row"),
        P(),
        P("gz", "gx", "row", None, None),
        P("gz", "gx", "row", None, None),
        P("gz", "gx", "row", None),
        P(("grp", "gz"), ("gx", "row"), None),
        P("gz", ("gx", "row"), None),
        P("gz", "gx", "row"),
    )

    return jax.shard_map(
        on_device,
        mesh=mesh,
        in_specs=placed,
        out_specs=P(("grp", "gz"), "gx", "row"),
        check_vma=False,
    )
```

```python
import functools
import math

import jax
import jax.numpy as jnp
from jax import lax
from jax.experimental import pallas as pl
from jax.experimental.pallas import tpu as pltpu
from jax.sharding import PartitionSpec as P

ONE_HOT = 256
GROUP = 8
STATIC_ROWS = 4096
VMEM_LIMIT = 16 * 1024 * 1024


def pack_kernel(
    window, target_in, weight_in, bid_in, vol_in, sends, bid, vox, target, weight, made, vol, sems
):
    pairs = ((vol_in, vol), (target_in, target), (weight_in, weight), (bid_in, bid))
    copies = [pltpu.make_async_copy(a, b, sems.at[i]) for i, (a, b) in enumerate(pairs)]
    for copy in copies:
        copy.start()
    made[...] = jnp.zeros_like(made)
    for copy in copies[1:]:
        copy.wait()
    slabs = sends.shape[0]
    depth = window - 2
    for s in range(slabs):
        low, high = max(s * depth - 1, 0), min(s * depth + depth + 1, slabs * depth)
        skip = low - (s * depth - 1)
        for own in range(target.shape[0]):
            for at, data in ((0, target), (made.shape[2] // 2, weight)):
                made[s, own, at + skip : at + skip + high - low, :] = data[own, low:high, :]
    sends[...] = made[...].astype(sends.dtype)
    copies[0].wait()
    lines, width = vol.shape
    tile = vox.shape[1]
    runs = width // tile
    step = 8
    for run in range(runs):
        for line in range(0, lines, step):
            vox[pl.ds(line * runs + run, step, stride=runs), :] = vol[
                line : line + step, run * tile : (run + 1) * tile
            ]


def forward_kernel(
    rows, live_in, tid_in, bid_in, vox, tiles_in, out, live, tid, bid, tiles, picked, sems
):
    angles, slots = tid.shape
    tile = tiles.shape[1]
    pairs = ((bid_in, bid), (tiles_in, tiles), (live_in, live), (tid_in, tid))
    copies = [pltpu.make_async_copy(a, b, sems.at[i]) for i, (a, b) in enumerate(pairs)]
    for copy in copies:
        copy.start()
    copies[0].wait()

    def gather(a, at):
        for j in range(slots * rows):
            picked[at + j : at + j + 1, :] = vox[pl.ds(bid[a, j], 1), :]

    def project(a, at):
        count = live[a]
        total = jnp.zeros((rows, tile), jnp.float32)
        for g in range(0, slots, GROUP):
            left, right = [], []
            for k in range(g, g + GROUP):
                part = picked[at + k * rows : at + (k + 1) * rows, :]
                left.append(jnp.where(k < count, part, 0.0).astype(jnp.bfloat16))
                right.append(tiles[tid[a, k]])
            total += lax.dot_general(
                jnp.concatenate(left, axis=1),
                jnp.concatenate(right, axis=1),
                (((1,), (1,)), ((), ())),
                preferred_element_type=jnp.float32,
            )
        return total

    length = slots * rows
    if angles * length <= STATIC_ROWS:
        ahead = min(2, angles)
        gather(0, 0)
        if ahead > 1:

            @pl.when(bid[0, 0] >= 0)
            def _():
                gather(1, length)

        for copy in copies[1:]:
            copy.wait()
        for a in range(angles):

            @pl.when(live[a] >= 0)
            def _():
                if a + ahead < angles:
                    gather(a + ahead, (a + ahead) % 3 * length)
                out[a * rows : (a + 1) * rows, :] = project(a, a % 3 * length)

    else:
        for copy in copies[1:]:
            copy.wait()

        def project_angle(a, carry):
            gather(a, 0)
            out[pl.ds(pl.multiple_of(a * rows, 8), rows), :] = project(a, 0)
            return carry

        lax.fori_loop(0, angles, project_angle, 0)


def backward_kernel(
    rows, joined, live, tid, bid, head, middle, tail, columns, tiles, vol_in, col_in, out_in,
    target, weight, res, hot, code, spread, vol, col, out, total, sems,
):
    angles, slots = tid.shape
    tile = tiles.shape[1]
    lines, width = vol.shape
    runs = width // tile
    high = hot.shape[0]
    length = slots * rows
    reads = [
        pltpu.make_async_copy(vol_in, vol, sems.at[0]),
        pltpu.make_async_copy(col_in, col, sems.at[1]),
    ]
    for copy in reads:
        copy.start()
    if joined:
        count = columns.shape[0]
        window = rows // count
        padded = columns.shape[1] // angles // 2
        for q in range(count):
            for a in range(angles):
                there = pl.ds(a * rows + q, window, stride=count)
                at = a * 2 * padded
                both = columns[q, at : at + 2 * padded, :].astype(jnp.float32)
                target[there, :] = both[:window]
                weight[there, :] = both[padded : padded + window]
    else:
        target[...] = columns[0].astype(jnp.float32)
        weight[...] = columns[1].astype(jnp.float32)
    for a in range(angles):
        parts = []
        for part in (head, middle, tail):
            size = part.shape[0] // angles
            parts.append(part[a * size : (a + 1) * size, :])
        here = slice(a * rows, (a + 1) * rows)
        error = target[here, :] - jnp.concatenate(parts, axis=0)
        res[a] = (weight[here, :] * error).astype(jnp.bfloat16)

    place = lax.broadcasted_iota(jnp.int32, (high, tile), 0).astype(jnp.bfloat16)
    position = lax.broadcasted_iota(jnp.int32, (1, tile), 1)
    static = angles * length <= STATIC_ROWS
    codes = []
    for a in range(angles):
        groups = []
        for c in range(0, length, tile):
            block = bid[a : a + 1, c : c + tile]
            line = block // runs
            low = (line % high).astype(jnp.bfloat16)
            hot[:, a * length + c : a * length + c + tile] = jnp.where(
                place == low, jnp.bfloat16(1), jnp.bfloat16(0)
            )
            group = (line // high) * runs + block % runs
            groups.append(jnp.where(position + c < live[a] * rows, group, -1))
        pad = -len(groups) % 8
        groups += [jnp.zeros((1, tile), jnp.int32)] * pad
        turned = jnp.concatenate(groups, axis=0).astype(jnp.float32).T
        for i in range(length // tile):
            wide = jnp.broadcast_to(turned[:, i : i + 1], (tile, tile))
            if static:
                codes.append(wide.astype(jnp.bfloat16))
            else:
                here = slice(a * length + i * tile, a * length + (i + 1) * tile)
                code[here, :] = wide.astype(jnp.bfloat16)

    def spread_pair(values, a, k):
        pair = jnp.concatenate([tiles[tid[a, k]], tiles[tid[a, k + 1]]], axis=1)
        made = jnp.dot(values, pair, preferred_element_type=jnp.float32)
        both = jnp.concatenate([made[:, :tile], made[:, tile:]], axis=0)
        return both.astype(jnp.bfloat16)

    def add_part(values, groups, chosen):
        right = jnp.concatenate(
            [
                jnp.where(groups == jnp.bfloat16(g), values, jnp.bfloat16(0))
                for g in range(chunks * runs)
            ],
            axis=1,
        )
        return jnp.dot(chosen, right, preferred_element_type=jnp.float32)

    chunks = lines // high
    writes = []

    def finish(first, count, made):
        for i in range(count):
            here = pl.ds((first + i) * high, high)
            out[here, :] = vol[here, :] + col[here, :] * made[:, i * width : (i + 1) * width]
            copy = pltpu.make_async_copy(
                out.at[here, :], out_in.at[here, :], sems.at[2 + first + i]
            )
            copy.start()
            writes.append(copy)

    if static:
        values = []
        for a in range(angles):
            for k in range(0, slots, 2):
                values.append(spread_pair(res[a], a, k))
        made = add_part(
            jnp.concatenate(values, axis=0), jnp.concatenate(codes, axis=0), hot[...]
        )
        for copy in reads:
            copy.wait()
        finish(0, chunks, made)
    else:

        def step(a, carry):
            values = res[a]
            base = pl.multiple_of(a * length, 256)
            for k in range(0, slots, 2):
                spread[k * rows : (k + 2) * rows, :] = spread_pair(values, a, k)
            total[...] += add_part(
                spread[...], code[pl.ds(base, length), :], hot[:, pl.ds(base, length)]
            )
            return carry

        total[...] = jnp.zeros_like(total)
        lax.fori_loop(0, angles, step, 0)
        for copy in reads:
            copy.wait()
        finish(0, chunks, total[...])
    for copy in writes:
        copy.wait()


def swap(values, axis, bit):
    return lax.ppermute(values, axis, [(i, i ^ bit) for i in range(lax.axis_size(axis))])


def move_many(arrays, axis, hops):
    if len({array.shape[-1] for array in arrays}) > 1:
        return [lax.ppermute(array, axis, hops) for array in arrays]
    width = arrays[0].shape[-1]
    joined = jnp.concatenate([a.reshape(-1, width) for a in arrays], axis=0)
    came = lax.ppermute(joined, axis, hops)
    out, at = [], 0
    for array in arrays:
        count = array.size // width
        out.append(came[at : at + count].reshape(array.shape))
        at += count
    return out


def swap_many(arrays, axis, bit):
    return move_many(arrays, axis, [(i, i ^ bit) for i in range(lax.axis_size(axis))])


def bits(axis):
    return [1 << i for i in range((lax.axis_size(axis) - 1).bit_length())]


def ordered(mine_high, own, other, axis):
    return jnp.concatenate(
        [jnp.where(mine_high, other, own), jnp.where(mine_high, own, other)], axis=axis
    )


def exchange_slabs(parts, bit):
    high = (lax.axis_index("gz") & bit) != 0
    count = parts.shape[0] // 2
    halves = parts.reshape((2, count) + parts.shape[1:])
    keep = jnp.where(high, halves[1], halves[0])
    give = jnp.where(high, halves[0], halves[1])
    with jax.named_scope(f"slab{bit}"):
        came = swap(give, "gz", bit)
    low, up = jnp.where(high, came, keep), jnp.where(high, keep, came)
    both = jnp.stack([low, up], axis=2)
    return both.reshape((count, parts.shape[1] * 2) + parts.shape[2:])


def on_device(volume, tile_table, tile_ids, block_ids, live_slots, measured, row_norm, col_norm):
    slab_depth, column_width, half_width = volume.shape
    tile_size = tile_table.shape[1]
    angle_count, slot_count = tile_ids.shape[3:]
    window = slab_depth + 2
    block_cols = block_ids.shape[4] // (slot_count * window)
    rows = window * block_cols
    rim = 2 * block_cols
    padded = -(-window // 8) * 8
    length = slot_count * rows
    lines = slab_depth * column_width
    runs = half_width // tile_size
    high = math.gcd(lines, ONE_HOT)
    slab_count = lax.axis_size("gz")
    own_angles, local_cols, row_total = measured.shape

    def held(array):
        return pltpu.with_memory_space_constraint(array, pltpu.HBM)

    tid = tile_ids.reshape(angle_count, slot_count)
    bid = block_ids.reshape(angle_count, length)
    live = live_slots.reshape(angle_count)
    vol = held(volume.reshape(lines, half_width))
    col = held(col_norm.reshape(lines, half_width))

    smem = pl.BlockSpec(memory_space=pltpu.SMEM)
    vmem = pl.BlockSpec(memory_space=pltpu.VMEM)
    hbm = pl.BlockSpec(memory_space=pltpu.HBM)
    params = pltpu.CompilerParams(vmem_limit_bytes=VMEM_LIMIT)
    buffers = 3 if angle_count * length <= STATIC_ROWS else 1

    sends, held_bid, vox = pl.pallas_call(
        functools.partial(pack_kernel, window),
        out_shape=(
            jax.ShapeDtypeStruct((slab_count, own_angles, 2 * padded, local_cols), jnp.bfloat16),
            jax.ShapeDtypeStruct((angle_count, length), jnp.int32),
            jax.ShapeDtypeStruct((lines * runs, tile_size), jnp.float32),
        ),
        in_specs=[hbm] * 4,
        out_specs=(vmem, vmem, vmem),
        scratch_shapes=[
            pltpu.VMEM((own_angles, row_total, local_cols), jnp.float32),
            pltpu.VMEM((own_angles, row_total, local_cols), jnp.float32),
            pltpu.VMEM((slab_count, own_angles, 2 * padded, local_cols), jnp.float32),
            pltpu.VMEM((lines, half_width), jnp.float32),
            pltpu.SemaphoreType.DMA((4,)),
        ],
        compiler_params=params,
        name="pack",
    )(held(measured.transpose(0, 2, 1)), held(row_norm.transpose(0, 2, 1)), held(bid), vol)
    columns = sends[:, None]
    for bit in bits("gz")[:0:-1]:
        columns = exchange_slabs(columns, bit)

    partial = pl.pallas_call(
        functools.partial(forward_kernel, rows),
        out_shape=jax.ShapeDtypeStruct((angle_count * rows, tile_size), jnp.float32),
        in_specs=[hbm, hbm, vmem, vmem, hbm],
        out_specs=vmem,
        scratch_shapes=[
            pltpu.SMEM((angle_count,), jnp.int32),
            pltpu.SMEM((angle_count, slot_count), jnp.int32),
            pltpu.SMEM((angle_count, length), jnp.int32),
            pltpu.VMEM(tile_table.shape, jnp.bfloat16),
            pltpu.VMEM((buffers * length, tile_size), jnp.float32),
            pltpu.SemaphoreType.DMA((4,)),
        ],
        compiler_params=params,
        name="forward",
    )(held(live), held(tid), held_bid, vox, held(tile_table))

    assert lax.axis_size("row") == 2
    upper = lax.axis_index("row") == 1
    odd = (lax.axis_index("gz") & 1) == 1
    top = upper != odd
    keep = jnp.where(odd, columns[1], columns[0])
    give = jnp.where(odd, columns[0], columns[1])
    columns = jnp.where(upper, give, keep)
    with jax.named_scope("rowsum"):
        passed = jnp.where(upper, keep, give).astype(jnp.float32)
        came = swap_many([partial, passed], "row", 1)
    total = partial + came[0]
    columns = ordered(upper, columns[None], came[1][None].astype(jnp.bfloat16), 0)[None]
    blocks = total.reshape(angle_count, rows, tile_size)
    outer = jnp.where(top, blocks[:, rows - rim :], blocks[:, :rim])
    middle = blocks[:, rim : rows - rim]
    for bit in bits("gx"):
        with jax.named_scope(f"gxsum{bit}"):
            parts = [outer.astype(jnp.bfloat16), middle.astype(jnp.bfloat16), columns]
            came = swap_many(parts, "gx", bit)
        outer = outer + came[0].astype(jnp.float32)
        middle = middle + came[1].astype(jnp.float32)
        columns = ordered((lax.axis_index("gx") & bit) != 0, columns, came[2], 0)
    hops = [(z * 2 + 1, (z ^ 1) * 2 + 1) for z in range(slab_count)]
    hops += [(z * 2, ((z + 1 ^ 1) - 1) * 2) for z in range(1, slab_count - 1)]
    with jax.named_scope("rims"):
        came = move_many([outer.astype(jnp.bfloat16), columns], ("gz", "row"), hops)
    outer = outer + came[0].astype(jnp.float32)
    columns = jnp.where(upper, came[1], columns)
    with jax.named_scope("finish"):
        came = swap_many([outer.astype(jnp.bfloat16), columns], "row", 1)
    far = came[0].astype(jnp.float32)
    head = jnp.where(top, far, outer).reshape(-1, tile_size)
    tail = jnp.where(top, outer, far).reshape(-1, tile_size)
    low, up = jnp.where(top, came[1], columns), jnp.where(top, columns, came[1])
    columns = jnp.stack([low, up], axis=3)
    joined = local_cols == tile_size
    if joined:
        columns = columns.reshape(block_cols, angle_count * 2 * padded, tile_size)
    else:
        columns = columns.reshape(-1, angle_count, 2, padded, local_cols)[:, :, :, :window]
        columns = columns.transpose(2, 1, 3, 0, 4).reshape(2, angle_count * rows, tile_size)

    made = pl.pallas_call(
        functools.partial(backward_kernel, rows, joined),
        out_shape=jax.ShapeDtypeStruct((lines, half_width), jnp.float32),
        in_specs=[smem, smem] + [vmem] * 6 + [hbm] * 2,
        out_specs=hbm,
        scratch_shapes=[
            pltpu.VMEM((angle_count * rows, tile_size), jnp.float32),
            pltpu.VMEM((angle_count * rows, tile_size), jnp.float32),
            pltpu.VMEM((angle_count, rows, tile_size), jnp.bfloat16),
            pltpu.VMEM((high, angle_count * length), jnp.bfloat16),
            pltpu.VMEM((angle_count * length, tile_size), jnp.bfloat16),
            pltpu.VMEM((length, tile_size), jnp.bfloat16),
            pltpu.VMEM((lines, half_width), jnp.float32),
            pltpu.VMEM((lines, half_width), jnp.float32),
            pltpu.VMEM((lines, half_width), jnp.float32),
            pltpu.VMEM((high, lines // high * half_width), jnp.float32),
            pltpu.SemaphoreType.DMA((2 + lines // high,)),
        ],
        compiler_params=params,
        name="backward",
    )(
        live, tid, bid, head, middle.reshape(-1, tile_size), tail, columns, tile_table, vol, col,
    )
    return made.reshape(slab_depth, column_width, half_width)


def solution(mesh):
    placed = (
        P(("grp", "gz"), "gx", "row"),
        P(),
        P("gz", "gx", "row", None, None),
        P("gz", "gx", "row", None, None),
        P("gz", "gx", "row", None),
        P(("grp", "gz"), ("gx", "row"), None),
        P("gz", ("gx", "row"), None),
        P("gz", "gx", "row"),
    )

    return jax.shard_map(
        on_device,
        mesh=mesh,
        in_specs=placed,
        out_specs=P(("grp", "gz"), "gx", "row"),
        check_vma=False,
    )
```

```python
import functools
import math

import jax
import jax.numpy as jnp
from jax import lax
from jax.experimental import pallas as pl
from jax.experimental.pallas import tpu as pltpu
from jax.sharding import PartitionSpec as P

ONE_HOT = 256
GROUP = 8
STATIC_ROWS = 4096
VMEM_LIMIT = 16 * 1024 * 1024


def pack_kernel(
    window, target_in, weight_in, bid_in, vol_in, sends, bid, vox, target, weight, made, vol, sems
):
    pairs = ((vol_in, vol), (target_in, target), (weight_in, weight), (bid_in, bid))
    copies = [pltpu.make_async_copy(a, b, sems.at[i]) for i, (a, b) in enumerate(pairs)]
    for copy in copies:
        copy.start()
    made[...] = jnp.zeros_like(made)
    for copy in copies[1:]:
        copy.wait()
    slabs = sends.shape[0]
    depth = window - 2
    for s in range(slabs):
        low, high = max(s * depth - 1, 0), min(s * depth + depth + 1, slabs * depth)
        skip = low - (s * depth - 1)
        for own in range(target.shape[0]):
            for at, data in ((0, target), (made.shape[2] // 2, weight)):
                made[s, own, at + skip : at + skip + high - low, :] = data[own, low:high, :]
    sends[...] = made[...].astype(sends.dtype)
    copies[0].wait()
    lines, width = vol.shape
    tile = vox.shape[1]
    runs = width // tile
    step = 8
    for run in range(runs):
        for line in range(0, lines, step):
            vox[pl.ds(line * runs + run, step, stride=runs), :] = vol[
                line : line + step, run * tile : (run + 1) * tile
            ]


def forward_kernel(
    rows, live_in, tid_in, bid_in, vox, tiles_in, out, tiles, live, tid, bid, picked, sems
):
    angles, slots = tid.shape
    tile = tiles.shape[1]
    pairs = ((bid_in, bid), (tiles_in, tiles), (live_in, live), (tid_in, tid))
    copies = [pltpu.make_async_copy(a, b, sems.at[i]) for i, (a, b) in enumerate(pairs)]
    for copy in copies:
        copy.start()
    copies[0].wait()

    def gather(a, at):
        for j in range(slots * rows):
            picked[at + j : at + j + 1, :] = vox[pl.ds(bid[a, j], 1), :]

    def project(a, at):
        count = live[a]
        total = jnp.zeros((rows, tile), jnp.float32)
        for g in range(0, slots, GROUP):
            left, right = [], []
            for k in range(g, g + GROUP):
                part = picked[at + k * rows : at + (k + 1) * rows, :]
                left.append(jnp.where(k < count, part, 0.0).astype(jnp.bfloat16))
                right.append(tiles[tid[a, k]])
            total += lax.dot_general(
                jnp.concatenate(left, axis=1),
                jnp.concatenate(right, axis=1),
                (((1,), (1,)), ((), ())),
                preferred_element_type=jnp.float32,
            )
        return total

    length = slots * rows
    if angles * length <= STATIC_ROWS:
        ahead = min(2, angles)
        gather(0, 0)
        if ahead > 1:

            @pl.when(bid[0, 0] >= 0)
            def _():
                gather(1, length)

        for copy in copies[1:]:
            copy.wait()
        for a in range(angles):

            @pl.when(live[a] >= 0)
            def _():
                if a + ahead < angles:
                    gather(a + ahead, (a + ahead) % 3 * length)
                out[a * rows : (a + 1) * rows, :] = project(a, a % 3 * length)

    else:
        for copy in copies[1:]:
            copy.wait()

        def project_angle(a, carry):
            gather(a, 0)
            out[pl.ds(pl.multiple_of(a * rows, 8), rows), :] = project(a, 0)
            return carry

        lax.fori_loop(0, angles, project_angle, 0)


def backward_kernel(
    rows, joined, live, tid, bid, head, middle, tail, columns, tiles, vol_in, col_in, out_in,
    target, weight, res, hot, code, spread, vol, col, out, total, sems,
):
    angles, slots = tid.shape
    tile = tiles.shape[1]
    lines, width = vol.shape
    runs = width // tile
    high = hot.shape[0]
    length = slots * rows
    reads = [
        pltpu.make_async_copy(vol_in, vol, sems.at[0]),
        pltpu.make_async_copy(col_in, col, sems.at[1]),
    ]
    for copy in reads:
        copy.start()
    if joined:
        count = columns.shape[0]
        window = rows // count
        padded = columns.shape[1] // angles // 2
        for q in range(count):
            for a in range(angles):
                there = pl.ds(a * rows + q, window, stride=count)
                at = a * 2 * padded
                both = columns[q, at : at + 2 * padded, :].astype(jnp.float32)
                target[there, :] = both[:window]
                weight[there, :] = both[padded : padded + window]
    else:
        target[...] = columns[0].astype(jnp.float32)
        weight[...] = columns[1].astype(jnp.float32)
    for a in range(angles):
        parts = []
        for part in (head, middle, tail):
            size = part.shape[0] // angles
            parts.append(part[a * size : (a + 1) * size, :])
        here = slice(a * rows, (a + 1) * rows)
        error = target[here, :] - jnp.concatenate(parts, axis=0)
        res[a] = (weight[here, :] * error).astype(jnp.bfloat16)

    place = lax.broadcasted_iota(jnp.int32, (high, tile), 0).astype(jnp.bfloat16)
    position = lax.broadcasted_iota(jnp.int32, (1, tile), 1)
    static = angles * length <= STATIC_ROWS
    codes = []
    for a in range(angles):
        groups = []
        for c in range(0, length, tile):
            block = bid[a : a + 1, c : c + tile]
            line = block // runs
            low = (line % high).astype(jnp.bfloat16)
            hot[:, a * length + c : a * length + c + tile] = jnp.where(
                place == low, jnp.bfloat16(1), jnp.bfloat16(0)
            )
            group = (line // high) * runs + block % runs
            groups.append(jnp.where(position + c < live[a] * rows, group, -1))
        pad = -len(groups) % 8
        groups += [jnp.zeros((1, tile), jnp.int32)] * pad
        turned = jnp.concatenate(groups, axis=0).astype(jnp.float32).T
        for i in range(length // tile):
            wide = jnp.broadcast_to(turned[:, i : i + 1], (tile, tile))
            if static:
                codes.append(wide.astype(jnp.bfloat16))
            else:
                here = slice(a * length + i * tile, a * length + (i + 1) * tile)
                code[here, :] = wide.astype(jnp.bfloat16)

    def spread_pair(values, a, k):
        pair = jnp.concatenate([tiles[tid[a, k]], tiles[tid[a, k + 1]]], axis=1)
        made = jnp.dot(values, pair, preferred_element_type=jnp.float32)
        both = jnp.concatenate([made[:, :tile], made[:, tile:]], axis=0)
        return both.astype(jnp.bfloat16)

    def add_part(values, groups, chosen):
        right = jnp.concatenate(
            [
                jnp.where(groups == jnp.bfloat16(g), values, jnp.bfloat16(0))
                for g in range(chunks * runs)
            ],
            axis=1,
        )
        return jnp.dot(chosen, right, preferred_element_type=jnp.float32)

    chunks = lines // high
    writes = []

    def finish(first, count, made):
        for i in range(count):
            here = pl.ds((first + i) * high, high)
            out[here, :] = vol[here, :] + col[here, :] * made[:, i * width : (i + 1) * width]
            copy = pltpu.make_async_copy(
                out.at[here, :], out_in.at[here, :], sems.at[2 + first + i]
            )
            copy.start()
            writes.append(copy)

    if static:
        values = []
        for a in range(angles):
            for k in range(0, slots, 2):
                values.append(spread_pair(res[a], a, k))
        made = add_part(
            jnp.concatenate(values, axis=0), jnp.concatenate(codes, axis=0), hot[...]
        )
        for copy in reads:
            copy.wait()
        finish(0, chunks, made)
    else:

        def step(a, carry):
            values = res[a]
            base = pl.multiple_of(a * length, 256)
            for k in range(0, slots, 2):
                spread[k * rows : (k + 2) * rows, :] = spread_pair(values, a, k)
            total[...] += add_part(
                spread[...], code[pl.ds(base, length), :], hot[:, pl.ds(base, length)]
            )
            return carry

        total[...] = jnp.zeros_like(total)
        lax.fori_loop(0, angles, step, 0)
        for copy in reads:
            copy.wait()
        finish(0, chunks, total[...])
    for copy in writes:
        copy.wait()


def swap(values, axis, bit):
    return lax.ppermute(values, axis, [(i, i ^ bit) for i in range(lax.axis_size(axis))])


def move_many(arrays, axis, hops):
    if len({array.shape[-1] for array in arrays}) > 1:
        return [lax.ppermute(array, axis, hops) for array in arrays]
    width = arrays[0].shape[-1]
    joined = jnp.concatenate([a.reshape(-1, width) for a in arrays], axis=0)
    came = lax.ppermute(joined, axis, hops)
    out, at = [], 0
    for array in arrays:
        count = array.size // width
        out.append(came[at : at + count].reshape(array.shape))
        at += count
    return out


def swap_many(arrays, axis, bit):
    return move_many(arrays, axis, [(i, i ^ bit) for i in range(lax.axis_size(axis))])


def bits(axis):
    return [1 << i for i in range((lax.axis_size(axis) - 1).bit_length())]


def ordered(mine_high, own, other, axis):
    return jnp.concatenate(
        [jnp.where(mine_high, other, own), jnp.where(mine_high, own, other)], axis=axis
    )


def exchange_slabs(parts, bit):
    high = (lax.axis_index("gz") & bit) != 0
    count = parts.shape[0] // 2
    halves = parts.reshape((2, count) + parts.shape[1:])
    keep = jnp.where(high, halves[1], halves[0])
    give = jnp.where(high, halves[0], halves[1])
    with jax.named_scope(f"slab{bit}"):
        came = swap(give, "gz", bit)
    low, up = jnp.where(high, came, keep), jnp.where(high, keep, came)
    both = jnp.stack([low, up], axis=2)
    return both.reshape((count, parts.shape[1] * 2) + parts.shape[2:])


def on_device(volume, tile_table, tile_ids, block_ids, live_slots, measured, row_norm, col_norm):
    slab_depth, column_width, half_width = volume.shape
    tile_size = tile_table.shape[1]
    angle_count, slot_count = tile_ids.shape[3:]
    window = slab_depth + 2
    block_cols = block_ids.shape[4] // (slot_count * window)
    rows = window * block_cols
    rim = 2 * block_cols
    padded = -(-window // 8) * 8
    length = slot_count * rows
    lines = slab_depth * column_width
    runs = half_width // tile_size
    high = math.gcd(lines, ONE_HOT)
    slab_count = lax.axis_size("gz")
    own_angles, local_cols, row_total = measured.shape

    def held(array):
        return pltpu.with_memory_space_constraint(array, pltpu.HBM)

    tid = tile_ids.reshape(angle_count, slot_count)
    bid = block_ids.reshape(angle_count, length)
    live = live_slots.reshape(angle_count)
    vol = held(volume.reshape(lines, half_width))
    col = held(col_norm.reshape(lines, half_width))

    smem = pl.BlockSpec(memory_space=pltpu.SMEM)
    vmem = pl.BlockSpec(memory_space=pltpu.VMEM)
    hbm = pl.BlockSpec(memory_space=pltpu.HBM)
    params = pltpu.CompilerParams(vmem_limit_bytes=VMEM_LIMIT)
    buffers = 3 if angle_count * length <= STATIC_ROWS else 1

    sends, held_bid, vox = pl.pallas_call(
        functools.partial(pack_kernel, window),
        out_shape=(
            jax.ShapeDtypeStruct((slab_count, own_angles, 2 * padded, local_cols), jnp.bfloat16),
            jax.ShapeDtypeStruct((angle_count, length), jnp.int32),
            jax.ShapeDtypeStruct((lines * runs, tile_size), jnp.float32),
        ),
        in_specs=[hbm] * 4,
        out_specs=(vmem, vmem, vmem),
        scratch_shapes=[
            pltpu.VMEM((own_angles, row_total, local_cols), jnp.float32),
            pltpu.VMEM((own_angles, row_total, local_cols), jnp.float32),
            pltpu.VMEM((slab_count, own_angles, 2 * padded, local_cols), jnp.float32),
            pltpu.VMEM((lines, half_width), jnp.float32),
            pltpu.SemaphoreType.DMA((4,)),
        ],
        compiler_params=params,
        name="pack",
    )(held(measured.transpose(0, 2, 1)), held(row_norm.transpose(0, 2, 1)), held(bid), vol)
    columns = sends[:, None]
    for bit in bits("gz")[:0:-1]:
        columns = exchange_slabs(columns, bit)

    partial, held_tiles = pl.pallas_call(
        functools.partial(forward_kernel, rows),
        out_shape=(
            jax.ShapeDtypeStruct((angle_count * rows, tile_size), jnp.float32),
            jax.ShapeDtypeStruct(tile_table.shape, tile_table.dtype),
        ),
        in_specs=[hbm, hbm, vmem, vmem, hbm],
        out_specs=(vmem, vmem),
        scratch_shapes=[
            pltpu.SMEM((angle_count,), jnp.int32),
            pltpu.SMEM((angle_count, slot_count), jnp.int32),
            pltpu.SMEM((angle_count, length), jnp.int32),
            pltpu.VMEM((buffers * length, tile_size), jnp.float32),
            pltpu.SemaphoreType.DMA((4,)),
        ],
        compiler_params=params,
        name="forward",
    )(held(live), held(tid), held_bid, vox, held(tile_table))

    assert lax.axis_size("row") == 2
    upper = lax.axis_index("row") == 1
    odd = (lax.axis_index("gz") & 1) == 1
    top = upper != odd
    keep = jnp.where(odd, columns[1], columns[0])
    give = jnp.where(odd, columns[0], columns[1])
    columns = jnp.where(upper, give, keep)
    with jax.named_scope("rowsum"):
        passed = jnp.where(upper, keep, give).astype(jnp.float32)
        came = swap_many([partial, passed], "row", 1)
    total = partial + came[0]
    columns = ordered(upper, columns[None], came[1][None].astype(jnp.bfloat16), 0)[None]
    blocks = total.reshape(angle_count, rows, tile_size)
    outer = jnp.where(top, blocks[:, rows - rim :], blocks[:, :rim])
    middle = blocks[:, rim : rows - rim]
    for bit in bits("gx"):
        with jax.named_scope(f"gxsum{bit}"):
            parts = [outer.astype(jnp.bfloat16), middle.astype(jnp.bfloat16), columns]
            came = swap_many(parts, "gx", bit)
        outer = outer + came[0].astype(jnp.float32)
        middle = middle + came[1].astype(jnp.float32)
        columns = ordered((lax.axis_index("gx") & bit) != 0, columns, came[2], 0)
    hops = [(z * 2 + 1, (z ^ 1) * 2 + 1) for z in range(slab_count)]
    hops += [(z * 2, ((z + 1 ^ 1) - 1) * 2) for z in range(1, slab_count - 1)]
    with jax.named_scope("rims"):
        came = move_many([outer.astype(jnp.bfloat16), columns], ("gz", "row"), hops)
    outer = outer + came[0].astype(jnp.float32)
    columns = jnp.where(upper, came[1], columns)
    with jax.named_scope("finish"):
        came = swap_many([outer.astype(jnp.bfloat16), columns], "row", 1)
    far = came[0].astype(jnp.float32)
    head = jnp.where(top, far, outer).reshape(-1, tile_size)
    tail = jnp.where(top, outer, far).reshape(-1, tile_size)
    low, up = jnp.where(top, came[1], columns), jnp.where(top, columns, came[1])
    columns = jnp.stack([low, up], axis=3)
    joined = local_cols == tile_size
    if joined:
        columns = columns.reshape(block_cols, angle_count * 2 * padded, tile_size)
    else:
        columns = columns.reshape(-1, angle_count, 2, padded, local_cols)[:, :, :, :window]
        columns = columns.transpose(2, 1, 3, 0, 4).reshape(2, angle_count * rows, tile_size)

    made = pl.pallas_call(
        functools.partial(backward_kernel, rows, joined),
        out_shape=jax.ShapeDtypeStruct((lines, half_width), jnp.float32),
        in_specs=[smem, smem] + [vmem] * 6 + [hbm] * 2,
        out_specs=hbm,
        scratch_shapes=[
            pltpu.VMEM((angle_count * rows, tile_size), jnp.float32),
            pltpu.VMEM((angle_count * rows, tile_size), jnp.float32),
            pltpu.VMEM((angle_count, rows, tile_size), jnp.bfloat16),
            pltpu.VMEM((high, angle_count * length), jnp.bfloat16),
            pltpu.VMEM((angle_count * length, tile_size), jnp.bfloat16),
            pltpu.VMEM((length, tile_size), jnp.bfloat16),
            pltpu.VMEM((lines, half_width), jnp.float32),
            pltpu.VMEM((lines, half_width), jnp.float32),
            pltpu.VMEM((lines, half_width), jnp.float32),
            pltpu.VMEM((high, lines // high * half_width), jnp.float32),
            pltpu.SemaphoreType.DMA((2 + lines // high,)),
        ],
        compiler_params=params,
        name="backward",
    )(
        live, tid, bid, head, middle.reshape(-1, tile_size), tail, columns, held_tiles, vol, col,
    )
    return made.reshape(slab_depth, column_width, half_width)


def solution(mesh):
    placed = (
        P(("grp", "gz"), "gx", "row"),
        P(),
        P("gz", "gx", "row", None, None),
        P("gz", "gx", "row", None, None),
        P("gz", "gx", "row", None),
        P(("grp", "gz"), ("gx", "row"), None),
        P("gz", ("gx", "row"), None),
        P("gz", "gx", "row"),
    )

    return jax.shard_map(
        on_device,
        mesh=mesh,
        in_specs=placed,
        out_specs=P(("grp", "gz"), "gx", "row"),
        check_vma=False,
    )
```

```python
import functools
import math

import jax
import jax.numpy as jnp
from jax import lax
from jax.experimental import pallas as pl
from jax.experimental.pallas import tpu as pltpu
from jax.sharding import PartitionSpec as P

ONE_HOT = 256
GROUP = 8
STATIC_ROWS = 4096
VMEM_LIMIT = 16 * 1024 * 1024


def pack_kernel(
    window, target_in, weight_in, bid_in, vol_in, sends, bid, vox, target, weight, made, vol, sems
):
    pairs = ((vol_in, vol), (target_in, target), (weight_in, weight), (bid_in, bid))
    copies = [pltpu.make_async_copy(a, b, sems.at[i]) for i, (a, b) in enumerate(pairs)]
    for copy in copies:
        copy.start()
    made[...] = jnp.zeros_like(made)
    for copy in copies[1:]:
        copy.wait()
    slabs = sends.shape[0]
    depth = window - 2
    for s in range(slabs):
        low, high = max(s * depth - 1, 0), min(s * depth + depth + 1, slabs * depth)
        skip = low - (s * depth - 1)
        for own in range(target.shape[0]):
            for at, data in ((0, target), (made.shape[2] // 2, weight)):
                made[s, own, at + skip : at + skip + high - low, :] = data[own, low:high, :]
    sends[...] = made[...].astype(sends.dtype)
    copies[0].wait()
    lines, width = vol.shape
    tile = vox.shape[1]
    runs = width // tile
    step = 8
    for run in range(runs):
        for line in range(0, lines, step):
            vox[pl.ds(line * runs + run, step, stride=runs), :] = vol[
                line : line + step, run * tile : (run + 1) * tile
            ]


def forward_kernel(
    rows, live_in, tid_in, bid_in, vox, tiles_in, out, tiles, live, tid, bid, picked, sems
):
    angles, slots = tid.shape
    tile = tiles.shape[1]
    pairs = ((bid_in, bid), (tiles_in, tiles), (live_in, live), (tid_in, tid))
    copies = [pltpu.make_async_copy(a, b, sems.at[i]) for i, (a, b) in enumerate(pairs)]
    for copy in copies:
        copy.start()
    copies[0].wait()

    def gather(a, at):
        for j in range(slots * rows):
            picked[at + j : at + j + 1, :] = vox[pl.ds(bid[a, j], 1), :]

    def project(a, at):
        count = live[a]
        total = jnp.zeros((rows, tile), jnp.float32)
        for g in range(0, slots, GROUP):
            left, right = [], []
            for k in range(g, g + GROUP):
                part = picked[at + k * rows : at + (k + 1) * rows, :]
                left.append(jnp.where(k < count, part, 0.0).astype(jnp.bfloat16))
                right.append(tiles[tid[a, k]])
            total += lax.dot_general(
                jnp.concatenate(left, axis=1),
                jnp.concatenate(right, axis=1),
                (((1,), (1,)), ((), ())),
                preferred_element_type=jnp.float32,
            )
        return total

    length = slots * rows
    if angles * length <= STATIC_ROWS:
        ahead = min(2, angles)
        gather(0, 0)
        if ahead > 1:

            @pl.when(bid[0, 0] >= 0)
            def _():
                gather(1, length)

        for copy in copies[1:]:
            copy.wait()
        for a in range(angles - ahead):

            @pl.when(live[a] >= 0)
            def _():
                gather(a + ahead, (a + ahead) % 3 * length)
                out[a * rows : (a + 1) * rows, :] = project(a, a % 3 * length)

        @pl.when(live[0] >= 0)
        def _():
            for a in range(angles - ahead, angles):
                out[a * rows : (a + 1) * rows, :] = project(a, a % 3 * length)

    else:
        for copy in copies[1:]:
            copy.wait()

        def project_angle(a, carry):
            gather(a, 0)
            out[pl.ds(pl.multiple_of(a * rows, 8), rows), :] = project(a, 0)
            return carry

        lax.fori_loop(0, angles, project_angle, 0)


def backward_kernel(
    rows, joined, live, tid, bid, head, middle, tail, columns, tiles, vol_in, col_in, out_in,
    target, weight, res, hot, code, spread, vol, col, out, total, sems,
):
    angles, slots = tid.shape
    tile = tiles.shape[1]
    lines, width = vol.shape
    runs = width // tile
    high = hot.shape[0]
    length = slots * rows
    reads = [
        pltpu.make_async_copy(vol_in, vol, sems.at[0]),
        pltpu.make_async_copy(col_in, col, sems.at[1]),
    ]
    for copy in reads:
        copy.start()
    if joined:
        count = columns.shape[0]
        window = rows // count
        padded = columns.shape[1] // angles // 2
        for q in range(count):
            for a in range(angles):
                there = pl.ds(a * rows + q, window, stride=count)
                at = a * 2 * padded
                both = columns[q, at : at + 2 * padded, :].astype(jnp.float32)
                target[there, :] = both[:window]
                weight[there, :] = both[padded : padded + window]
    else:
        target[...] = columns[0].astype(jnp.float32)
        weight[...] = columns[1].astype(jnp.float32)
    for a in range(angles):
        parts = []
        for part in (head, middle, tail):
            size = part.shape[0] // angles
            parts.append(part[a * size : (a + 1) * size, :])
        here = slice(a * rows, (a + 1) * rows)
        error = target[here, :] - jnp.concatenate(parts, axis=0)
        res[a] = (weight[here, :] * error).astype(jnp.bfloat16)

    place = lax.broadcasted_iota(jnp.int32, (high, tile), 0).astype(jnp.bfloat16)
    position = lax.broadcasted_iota(jnp.int32, (1, tile), 1)
    static = angles * length <= STATIC_ROWS
    codes = []
    for a in range(angles):
        groups = []
        for c in range(0, length, tile):
            block = bid[a : a + 1, c : c + tile]
            line = block // runs
            low = (line % high).astype(jnp.bfloat16)
            hot[:, a * length + c : a * length + c + tile] = jnp.where(
                place == low, jnp.bfloat16(1), jnp.bfloat16(0)
            )
            group = (line // high) * runs + block % runs
            groups.append(jnp.where(position + c < live[a] * rows, group, -1))
        pad = -len(groups) % 8
        groups += [jnp.zeros((1, tile), jnp.int32)] * pad
        turned = jnp.concatenate(groups, axis=0).astype(jnp.float32).T
        for i in range(length // tile):
            wide = jnp.broadcast_to(turned[:, i : i + 1], (tile, tile))
            if static:
                codes.append(wide.astype(jnp.bfloat16))
            else:
                here = slice(a * length + i * tile, a * length + (i + 1) * tile)
                code[here, :] = wide.astype(jnp.bfloat16)

    def spread_pair(values, a, k):
        pair = jnp.concatenate([tiles[tid[a, k]], tiles[tid[a, k + 1]]], axis=1)
        made = jnp.dot(values, pair, preferred_element_type=jnp.float32)
        both = jnp.concatenate([made[:, :tile], made[:, tile:]], axis=0)
        return both.astype(jnp.bfloat16)

    def add_part(values, groups, chosen):
        right = jnp.concatenate(
            [
                jnp.where(groups == jnp.bfloat16(g), values, jnp.bfloat16(0))
                for g in range(chunks * runs)
            ],
            axis=1,
        )
        return jnp.dot(chosen, right, preferred_element_type=jnp.float32)

    chunks = lines // high
    writes = []

    def finish(first, count, made):
        for i in range(count):
            here = pl.ds((first + i) * high, high)
            out[here, :] = vol[here, :] + col[here, :] * made[:, i * width : (i + 1) * width]
            copy = pltpu.make_async_copy(
                out.at[here, :], out_in.at[here, :], sems.at[2 + first + i]
            )
            copy.start()
            writes.append(copy)

    if static:
        values = []
        for a in range(angles):
            for k in range(0, slots, 2):
                values.append(spread_pair(res[a], a, k))
        made = add_part(
            jnp.concatenate(values, axis=0), jnp.concatenate(codes, axis=0), hot[...]
        )
        for copy in reads:
            copy.wait()
        finish(0, chunks, made)
    else:

        def step(a, carry):
            values = res[a]
            base = pl.multiple_of(a * length, 256)
            for k in range(0, slots, 2):
                spread[k * rows : (k + 2) * rows, :] = spread_pair(values, a, k)
            total[...] += add_part(
                spread[...], code[pl.ds(base, length), :], hot[:, pl.ds(base, length)]
            )
            return carry

        total[...] = jnp.zeros_like(total)
        lax.fori_loop(0, angles, step, 0)
        for copy in reads:
            copy.wait()
        finish(0, chunks, total[...])
    for copy in writes:
        copy.wait()


def swap(values, axis, bit):
    return lax.ppermute(values, axis, [(i, i ^ bit) for i in range(lax.axis_size(axis))])


def move_many(arrays, axis, hops):
    if len({array.shape[-1] for array in arrays}) > 1:
        return [lax.ppermute(array, axis, hops) for array in arrays]
    width = arrays[0].shape[-1]
    joined = jnp.concatenate([a.reshape(-1, width) for a in arrays], axis=0)
    came = lax.ppermute(joined, axis, hops)
    out, at = [], 0
    for array in arrays:
        count = array.size // width
        out.append(came[at : at + count].reshape(array.shape))
        at += count
    return out


def swap_many(arrays, axis, bit):
    return move_many(arrays, axis, [(i, i ^ bit) for i in range(lax.axis_size(axis))])


def bits(axis):
    return [1 << i for i in range((lax.axis_size(axis) - 1).bit_length())]


def ordered(mine_high, own, other, axis):
    return jnp.concatenate(
        [jnp.where(mine_high, other, own), jnp.where(mine_high, own, other)], axis=axis
    )


def exchange_slabs(parts, bit):
    high = (lax.axis_index("gz") & bit) != 0
    count = parts.shape[0] // 2
    halves = parts.reshape((2, count) + parts.shape[1:])
    keep = jnp.where(high, halves[1], halves[0])
    give = jnp.where(high, halves[0], halves[1])
    with jax.named_scope(f"slab{bit}"):
        came = swap(give, "gz", bit)
    low, up = jnp.where(high, came, keep), jnp.where(high, keep, came)
    both = jnp.stack([low, up], axis=2)
    return both.reshape((count, parts.shape[1] * 2) + parts.shape[2:])


def on_device(volume, tile_table, tile_ids, block_ids, live_slots, measured, row_norm, col_norm):
    slab_depth, column_width, half_width = volume.shape
    tile_size = tile_table.shape[1]
    angle_count, slot_count = tile_ids.shape[3:]
    window = slab_depth + 2
    block_cols = block_ids.shape[4] // (slot_count * window)
    rows = window * block_cols
    rim = 2 * block_cols
    padded = -(-window // 8) * 8
    length = slot_count * rows
    lines = slab_depth * column_width
    runs = half_width // tile_size
    high = math.gcd(lines, ONE_HOT)
    slab_count = lax.axis_size("gz")
    own_angles, local_cols, row_total = measured.shape

    def held(array):
        return pltpu.with_memory_space_constraint(array, pltpu.HBM)

    tid = tile_ids.reshape(angle_count, slot_count)
    bid = block_ids.reshape(angle_count, length)
    live = live_slots.reshape(angle_count)
    vol = held(volume.reshape(lines, half_width))
    col = held(col_norm.reshape(lines, half_width))

    smem = pl.BlockSpec(memory_space=pltpu.SMEM)
    vmem = pl.BlockSpec(memory_space=pltpu.VMEM)
    hbm = pl.BlockSpec(memory_space=pltpu.HBM)
    params = pltpu.CompilerParams(vmem_limit_bytes=VMEM_LIMIT)
    buffers = 3 if angle_count * length <= STATIC_ROWS else 1

    sends, held_bid, vox = pl.pallas_call(
        functools.partial(pack_kernel, window),
        out_shape=(
            jax.ShapeDtypeStruct((slab_count, own_angles, 2 * padded, local_cols), jnp.bfloat16),
            jax.ShapeDtypeStruct((angle_count, length), jnp.int32),
            jax.ShapeDtypeStruct((lines * runs, tile_size), jnp.float32),
        ),
        in_specs=[hbm] * 4,
        out_specs=(vmem, vmem, vmem),
        scratch_shapes=[
            pltpu.VMEM((own_angles, row_total, local_cols), jnp.float32),
            pltpu.VMEM((own_angles, row_total, local_cols), jnp.float32),
            pltpu.VMEM((slab_count, own_angles, 2 * padded, local_cols), jnp.float32),
            pltpu.VMEM((lines, half_width), jnp.float32),
            pltpu.SemaphoreType.DMA((4,)),
        ],
        compiler_params=params,
        name="pack",
    )(held(measured.transpose(0, 2, 1)), held(row_norm.transpose(0, 2, 1)), held(bid), vol)
    columns = sends[:, None]
    for bit in bits("gz")[:0:-1]:
        columns = exchange_slabs(columns, bit)

    partial, held_tiles = pl.pallas_call(
        functools.partial(forward_kernel, rows),
        out_shape=(
            jax.ShapeDtypeStruct((angle_count * rows, tile_size), jnp.float32),
            jax.ShapeDtypeStruct(tile_table.shape, tile_table.dtype),
        ),
        in_specs=[hbm, hbm, vmem, vmem, hbm],
        out_specs=(vmem, vmem),
        scratch_shapes=[
            pltpu.SMEM((angle_count,), jnp.int32),
            pltpu.SMEM((angle_count, slot_count), jnp.int32),
            pltpu.SMEM((angle_count, length), jnp.int32),
            pltpu.VMEM((buffers * length, tile_size), jnp.float32),
            pltpu.SemaphoreType.DMA((4,)),
        ],
        compiler_params=params,
        name="forward",
    )(held(live), held(tid), held_bid, vox, held(tile_table))

    assert lax.axis_size("row") == 2
    upper = lax.axis_index("row") == 1
    odd = (lax.axis_index("gz") & 1) == 1
    top = upper != odd
    keep = jnp.where(odd, columns[1], columns[0])
    give = jnp.where(odd, columns[0], columns[1])
    columns = jnp.where(upper, give, keep)
    with jax.named_scope("rowsum"):
        passed = jnp.where(upper, keep, give).astype(jnp.float32)
        came = swap_many([partial, passed], "row", 1)
    total = partial + came[0]
    columns = ordered(upper, columns[None], came[1][None].astype(jnp.bfloat16), 0)[None]
    blocks = total.reshape(angle_count, rows, tile_size)
    outer = jnp.where(top, blocks[:, rows - rim :], blocks[:, :rim])
    middle = blocks[:, rim : rows - rim]
    for bit in bits("gx"):
        with jax.named_scope(f"gxsum{bit}"):
            parts = [outer.astype(jnp.bfloat16), middle.astype(jnp.bfloat16), columns]
            came = swap_many(parts, "gx", bit)
        outer = outer + came[0].astype(jnp.float32)
        middle = middle + came[1].astype(jnp.float32)
        columns = ordered((lax.axis_index("gx") & bit) != 0, columns, came[2], 0)
    hops = [(z * 2 + 1, (z ^ 1) * 2 + 1) for z in range(slab_count)]
    hops += [(z * 2, ((z + 1 ^ 1) - 1) * 2) for z in range(1, slab_count - 1)]
    with jax.named_scope("rims"):
        came = move_many([outer.astype(jnp.bfloat16), columns], ("gz", "row"), hops)
    outer = outer + came[0].astype(jnp.float32)
    columns = jnp.where(upper, came[1], columns)
    with jax.named_scope("finish"):
        came = swap_many([outer.astype(jnp.bfloat16), columns], "row", 1)
    far = came[0].astype(jnp.float32)
    head = jnp.where(top, far, outer).reshape(-1, tile_size)
    tail = jnp.where(top, outer, far).reshape(-1, tile_size)
    low, up = jnp.where(top, came[1], columns), jnp.where(top, columns, came[1])
    columns = jnp.stack([low, up], axis=3)
    joined = local_cols == tile_size
    if joined:
        columns = columns.reshape(block_cols, angle_count * 2 * padded, tile_size)
    else:
        columns = columns.reshape(-1, angle_count, 2, padded, local_cols)[:, :, :, :window]
        columns = columns.transpose(2, 1, 3, 0, 4).reshape(2, angle_count * rows, tile_size)

    made = pl.pallas_call(
        functools.partial(backward_kernel, rows, joined),
        out_shape=jax.ShapeDtypeStruct((lines, half_width), jnp.float32),
        in_specs=[smem, smem] + [vmem] * 6 + [hbm] * 2,
        out_specs=hbm,
        scratch_shapes=[
            pltpu.VMEM((angle_count * rows, tile_size), jnp.float32),
            pltpu.VMEM((angle_count * rows, tile_size), jnp.float32),
            pltpu.VMEM((angle_count, rows, tile_size), jnp.bfloat16),
            pltpu.VMEM((high, angle_count * length), jnp.bfloat16),
            pltpu.VMEM((angle_count * length, tile_size), jnp.bfloat16),
            pltpu.VMEM((length, tile_size), jnp.bfloat16),
            pltpu.VMEM((lines, half_width), jnp.float32),
            pltpu.VMEM((lines, half_width), jnp.float32),
            pltpu.VMEM((lines, half_width), jnp.float32),
            pltpu.VMEM((high, lines // high * half_width), jnp.float32),
            pltpu.SemaphoreType.DMA((2 + lines // high,)),
        ],
        compiler_params=params,
        name="backward",
    )(
        live, tid, bid, head, middle.reshape(-1, tile_size), tail, columns, held_tiles, vol, col,
    )
    return made.reshape(slab_depth, column_width, half_width)


def solution(mesh):
    placed = (
        P(("grp", "gz"), "gx", "row"),
        P(),
        P("gz", "gx", "row", None, None),
        P("gz", "gx", "row", None, None),
        P("gz", "gx", "row", None),
        P(("grp", "gz"), ("gx", "row"), None),
        P("gz", ("gx", "row"), None),
        P("gz", "gx", "row"),
    )

    return jax.shard_map(
        on_device,
        mesh=mesh,
        in_specs=placed,
        out_specs=P(("grp", "gz"), "gx", "row"),
        check_vma=False,
    )
```
